512 devices in a mesh: groups: 2 (over y), seq: 16 (over z), head: 8 (over x), inner: 2 (over core).
Axes of the slice: x: 8, y: 2, z: 16, core: 2. Of those that a mesh axis runs over, the one named last changes fastest.
The devices are a block of a 8x16x16 slice.
Arguments:
- queries: bfloat16 [16384, 8, 8, 128], P(('groups', 'seq'), 'head', 'inner'), parts along dimension 0, may hold values from -120 to 120
- grad_out: bfloat16 [16384, 8, 8, 128], P(('groups', 'seq'), 'head', 'inner'), parts along dimension 0, may hold values from -6 to 6
- keys: bfloat16 [16384, 8, 128], P(('groups', 'seq'), 'head'), parts along dimension 0, may hold values from -6 to 6
- values: bfloat16 [16384, 8, 128], P(('groups', 'seq'), 'head'), parts along dimension 0, may hold values from -6 to 6
- indices: int32 [8, 256, 16], P('head', 'groups'), parts along dimension 1, may hold values from 0 to 127, as said below
- valid: int32 [8, 256, 16], P('head', 'groups'), parts along dimension 1, may hold values from 0 to 1
Outputs:
- grad_queries: bfloat16 [16384, 8, 8, 128], P(('groups', 'seq'), 'head', 'inner'), parts along dimension 0
- grad_keys: bfloat16 [16384, 8, 128], P(('groups', 'seq'), 'head'), parts along dimension 0
- grad_values: bfloat16 [16384, 8, 128], P(('groups', 'seq'), 'head'), parts along dimension 0
The draws below stay inside these ranges and needn't reach their ends.
There are 2 independent parts, one for each index of `groups`. The reference program is written for one: setup_inputs(seed, part) draws one part's arguments, and reference() takes and returns one part's arrays. A program takes and returns all parts, laid end to end along the dimension named above; each array names one. Nothing has to cross between parts.
Inputs may be any that keep to these rules, and one draw needn't show every extreme that they name: `indices`: call blocks r * 8 to r * 8 + 7 run r. For every KV head and query block b: slot 0 names b and is valid; the valid slots name distinct blocks at most b; over all query blocks of run r, the valid slots name blocks of runs later than r never, and for each earlier run exactly 4 distinct blocks of it. Slots that are not valid name arbitrary blocks.
All inputs are finite; a program needn't handle non-finite values.
Results may differ from the reference program's by a relative error of at most 0.007.
Values may be sent and summed in bfloat16 or wider, within the bound.
A program may use at most 64 MiB of HBM per device.

```python
import jax
import jax.numpy as jnp
from jax import lax

HD = 128
GQ = 8
KVH = 8
BLK = 64
TOPK = 16
CAP = 4
QBD = 8
NQB = 128
SEQ_LEN = 8192


def paired_fields(key):
    base = jax.random.fold_in(key, 11)
    query_key, other_key = jax.random.split(base)
    drawn_q = jnp.clip(jax.random.normal(query_key, (SEQ_LEN, KVH, GQ, HD), jnp.float32), -6.0, 6.0)
    drawn_k = jnp.clip(jax.random.normal(other_key, (SEQ_LEN, KVH, HD), jnp.float32), -6.0, 6.0)
    keys_out = drawn_k
    queries_out = drawn_q
    return (queries_out, keys_out)


def draw_queries(key, part):
    return paired_fields(key)[0].astype(jnp.bfloat16)


def draw_keys(key, part):
    return paired_fields(key)[1].astype(jnp.bfloat16)


def selection(key):
    base = jax.random.fold_in(key, 29)
    pool_key, noise_key, count_key = jax.random.split(base, 3)
    runs = NQB // QBD
    blocks = jnp.arange(NQB, dtype=jnp.int32)
    owner = blocks // QBD
    local = blocks % QBD
    pool_score = jax.random.randint(pool_key, (KVH, runs, runs, QBD), 0, 2 ** 20, jnp.int32) * QBD + jnp.arange(QBD, dtype=jnp.int32)
    order = jnp.argsort(-pool_score, axis=-1, stable=True)
    ranking = jnp.argsort(order, axis=-1, stable=True).astype(jnp.int32)
    in_pool = ranking < CAP
    pool_pair = in_pool[:, owner[:, None], owner[None, :], local[None, :]]
    pool_rank = ranking[:, owner[:, None], owner[None, :], local[None, :]]
    remote_ok = (owner[None, :] < owner[:, None])[None] & pool_pair
    own_ok = ((owner[None, :] == owner[:, None]) & (blocks[None, :] < blocks[:, None]))[None]
    is_self = (blocks[None, :] == blocks[:, None])[None]
    query_local = (blocks % QBD)[:, None][None]
    forced = remote_ok & ((owner[None, :] * CAP + pool_rank) % QBD == query_local)
    noise = jax.random.randint(noise_key, (KVH, NQB, NQB), 0, 2 ** 16, jnp.int32) * NQB + blocks
    score = noise + forced.astype(jnp.int32) * 2 ** 29 + is_self.astype(jnp.int32) * 2 ** 30
    score = jnp.where(is_self | own_ok | remote_ok, score, -1 - blocks)
    top_values, top_blocks = lax.top_k(score, TOPK)
    forced_count = jnp.sum(forced.astype(jnp.int32), axis=-1)
    drawn_count = jax.random.randint(count_key, (KVH, NQB), TOPK // 2, TOPK + 1, jnp.int32)
    keeping = jnp.maximum(drawn_count, 1 + forced_count)
    usable = (top_values >= 0) & (jnp.arange(TOPK, dtype=jnp.int32)[None, None, :] < keeping[..., None])
    return (top_blocks.astype(jnp.int32), usable.astype(jnp.int32))


def draw_indices(key, part):
    return selection(key)[0]


def draw_valid(key, part):
    return selection(key)[1]


def block_levels(rng, extent, cuts, low, high):
    loudness = 1.0
    for axis_at, blocks in cuts:
        draws = jax.random.uniform(jax.random.fold_in(jax.random.fold_in(rng, 6), axis_at), (blocks,), jnp.float32, low / len(cuts), high / len(cuts))
        loudness = loudness * jnp.repeat(jnp.exp(draws), extent[axis_at] // blocks).reshape((-1,) + (1,) * (len(extent) - 1 - axis_at))
    return loudness


def bell_draw(own_key, dims, deviation, limit, shards=(), kind=jnp.bfloat16):
    array = jax.random.normal(own_key, dims, jnp.float32) * deviation
    if len(shards) > 0:
        array = block_levels(own_key, dims, shards, -0.22, 0.18) * array
    return jnp.clip(array, min=-limit, max=limit).astype(kind)


def setup_inputs(seed: int = 0, part: int = 0) -> dict:
    arg_keys = jax.random.split(jax.random.key(seed), 7)
    part_splits = jax.random.split(jax.random.fold_in(arg_keys[6], part), 7)
    queries = draw_queries(jax.random.fold_in(jax.random.fold_in(arg_keys[6], part), 71), part)
    grad_out = bell_draw(part_splits[1], (SEQ_LEN, KVH, GQ, HD), 1.0, 6.0, ((0, 16), (1, 8), (2, 2)))
    keys = draw_keys(jax.random.fold_in(jax.random.fold_in(arg_keys[6], part), 71), part)
    values = bell_draw(part_splits[3], (SEQ_LEN, KVH, HD), 1.0, 6.0, ((0, 16), (1, 8)))
    indices = draw_indices(jax.random.fold_in(jax.random.fold_in(arg_keys[6], part), 71), part)
    valid = draw_valid(jax.random.fold_in(jax.random.fold_in(arg_keys[6], part), 71), part)
    return {"queries": queries, "grad_out": grad_out, "keys": keys, "values": values, "indices": indices, "valid": valid}


def reference(queries, grad_out, keys, values, indices, valid):
    scaling = 1.0 / jnp.sqrt(jnp.float32(HD))
    position = jnp.arange(BLK, dtype=jnp.int32)
    causal = position[None, :] <= position[:, None]

    def per_head(head):
        q_head = queries[:, head].reshape(NQB, BLK, GQ, HD)
        do_head = grad_out[:, head].reshape(NQB, BLK, GQ, HD)
        k_head = keys[:, head].reshape(NQB, BLK, HD)
        v_head = values[:, head].reshape(NQB, BLK, HD)

        def step(carry, inputs):
            key_acc, value_acc = carry
            q_block, do_block, picks, usable, block = inputs
            k_sel = k_head[picks].reshape(TOPK * BLK, HD).astype(jnp.float32)
            v_sel = v_head[picks].reshape(TOPK * BLK, HD).astype(jnp.float32)
            before = picks < block
            same = picks == block
            allowed = usable[None, :, None] & (before[None, :, None] | same[None, :, None] & causal[:, None, :])
            allowed = allowed.reshape(BLK, TOPK * BLK)[None]
            q_float = q_block.astype(jnp.float32)
            do_float = do_block.astype(jnp.float32)
            scores = jnp.einsum('igw,sw->gis', q_float, k_sel) * scaling
            highest = lax.optimization_barrier(jnp.max(jnp.where(allowed, scores, -jnp.inf), axis=-1, keepdims=True))
            weights = jnp.where(allowed, jnp.exp(scores - highest), 0.0)
            probs = weights / lax.optimization_barrier(jnp.sum(weights, axis=-1, keepdims=True))
            probs_b = probs.astype(jnp.bfloat16)
            dprobs = jnp.einsum('igw,sw->gis', do_float, v_sel)
            delta = lax.optimization_barrier(jnp.sum(probs * dprobs, axis=-1, keepdims=True))
            dscores = (probs * (dprobs - delta)).astype(jnp.bfloat16).astype(jnp.float32)
            grad_q = (jnp.einsum('gis,sw->igw', dscores, k_sel) * scaling).astype(jnp.bfloat16)
            key_terms = jnp.einsum('gis,igw->sw', dscores, q_float) * scaling
            value_terms = jnp.einsum('gis,igw->sw', probs_b.astype(jnp.float32), do_float)
            key_acc = key_acc.at[picks].add(key_terms.reshape(TOPK, BLK, HD))
            value_acc = value_acc.at[picks].add(value_terms.reshape(TOPK, BLK, HD))
            return ((key_acc, value_acc), grad_q)
        start = (jnp.zeros((NQB, BLK, HD), jnp.float32), jnp.zeros((NQB, BLK, HD), jnp.float32))
        inputs = (q_head, do_head, indices[head].astype(jnp.int32), valid[head] > 0, jnp.arange(NQB, dtype=jnp.int32))
        (key_acc, value_acc), grad_q = lax.scan(step, start, inputs)
        return (grad_q, key_acc.astype(jnp.bfloat16), value_acc.astype(jnp.bfloat16))
    grad_q, grad_k, grad_v = lax.map(per_head, jnp.arange(KVH, dtype=jnp.int32))
    grad_queries = grad_q.transpose(1, 2, 0, 3, 4).reshape(SEQ_LEN, KVH, GQ, HD)
    grad_keys = grad_k.transpose(1, 2, 0, 3).reshape(SEQ_LEN, KVH, HD)
    grad_values = grad_v.transpose(1, 2, 0, 3).reshape(SEQ_LEN, KVH, HD)
    return (grad_queries, grad_keys, grad_values)
```

```python
import functools
import math

import jax
import jax.numpy as jnp
from jax import lax
from jax.experimental import pallas as pl
from jax.experimental.pallas import tpu as pltpu
from jax.sharding import PartitionSpec as P

BLK = 64
TOPK = 16
SUB = 4
MESH = pl.DeviceIdType.MESH
LOG2E = 1.4426950408889634


def greet(axes_ids):
    barrier = pltpu.get_barrier_semaphore()
    for where in axes_ids:
        pl.semaphore_signal(barrier, inc=1, device_id=where, device_id_type=MESH)
    pl.semaphore_wait(barrier, len(axes_ids))


def places(n):
    me = lax.axis_index("seq")
    core = lax.axis_index("inner")
    up = {"seq": lax.rem(me + 1, n)}
    down = {"seq": lax.rem(me + n - 1, n)}
    partner = {"inner": 1 - core}
    return me, core, up, down, partner


def send(src, dst, s_sem, r_sem, where):
    return pltpu.make_async_remote_copy(
        src_ref=src, dst_ref=dst, send_sem=s_sem, recv_sem=r_sem, device_id=where, device_id_type=MESH
    )


def gather_kernel(n, k_ref, v_ref, kv_ref, local_sem, us, ur, ds, dr, ps, pr):
    me, core, up, down, partner = places(n)
    rows = k_ref.shape[0]
    part = rows // SUB
    n_up = n // 2
    n_down = n - 1 - n_up
    own_k = pltpu.make_async_copy(k_ref, kv_ref.at[0, me], local_sem.at[0])
    own_v = pltpu.make_async_copy(v_ref, kv_ref.at[1, me], local_sem.at[1])
    own_k.start()
    own_v.start()
    greet((up, down, partner))
    own_k.wait()
    own_v.wait()

    def piece(run, u):
        return kv_ref.at[core, run, pl.ds(u * part, part)]

    started = []

    def go_up(t, u):
        run = lax.rem(me - t + n, n)
        c = send(piece(run, u), piece(run, u), us.at[t * SUB + u], ur.at[t * SUB + u], up)
        c.start()
        started.append(c)
        return c

    def go_down(t, u):
        run = lax.rem(me + t, n)
        c = send(piece(run, u), piece(run, u), ds.at[t * SUB + u], dr.at[t * SUB + u], down)
        c.start()
        started.append(c)
        return c

    ups = [go_up(0, u) for u in range(SUB)]
    downs = [go_down(0, u) for u in range(SUB)]
    across = []

    def share(run, j):
        c = send(kv_ref.at[core, run], kv_ref.at[core, run], ps.at[j], pr.at[j], partner)
        c.start()
        across.append(c)

    for t in range(n_up):
        next_ups, next_downs = [], []
        for u in range(SUB):
            ups[u].wait_recv()
            if t + 1 < n_up:
                next_ups.append(go_up(t + 1, u))
            if t < n_down:
                downs[u].wait_recv()
                if t + 1 < n_down:
                    next_downs.append(go_down(t + 1, u))
        share(lax.rem(me - 1 - t + n, n), 2 * t)
        if t < n_down:
            share(lax.rem(me + 1 + t, n), 2 * t + 1)
        ups, downs = next_ups, next_downs
    for c in across:
        c.wait_recv()
    for c in started + across:
        c.wait_send()


def attend_kernel(scaling, picks, usable, q_ref, do_ref, kv_ref, dq_ref, mine_ref, theirs_ref, other):
    i = pl.program_id(0)
    core = lax.axis_index("inner")
    first = core == 0
    rows = q_ref.shape[0]
    per_pos = rows // BLK

    @pl.when(i == 0)
    def _():
        mine_ref[...] = jnp.zeros_like(mine_ref)
        other[...] = jnp.zeros_like(other)

    q = q_ref[...]
    do = do_ref[...]
    names = [picks[i, t] for t in range(TOPK)]
    ks = jnp.concatenate([kv_ref[0, b] for b in names], axis=0)
    vs = jnp.concatenate([kv_ref[1, b] for b in names], axis=0)
    nt = (((1,), (1,)), ((), ()))
    st = lax.dot_general(ks, q, nt, preferred_element_type=jnp.float32)
    key_at = lax.broadcasted_iota(jnp.int32, (BLK, rows), 0)
    query_at = lax.broadcasted_iota(jnp.int32, (BLK, rows), 1) // per_pos
    low = jnp.float32(-1e30)
    parts = [jnp.where(key_at <= query_at, st[:BLK], low)]
    for t in range(1, TOPK):
        bias = jnp.where(usable[i, t] > 0, jnp.float32(0.0), low)
        parts.append(st[t * BLK : (t + 1) * BLK] + bias)
    st = jnp.concatenate(parts, axis=0)
    top = jnp.max(st, axis=0, keepdims=True)
    w = jnp.exp2((st - top) * jnp.float32(scaling * LOG2E))
    inv = 1.0 / jnp.sum(w, axis=0, keepdims=True)
    p = w * inv
    dp = lax.dot_general(vs, do, nt, preferred_element_type=jnp.float32)
    delta = jnp.sum(p * dp, axis=0, keepdims=True)
    dsc = (p * (dp - delta)).astype(jnp.bfloat16)
    pb = p.astype(jnp.bfloat16)
    dqt = lax.dot_general(ks, dsc, (((0,), (0,)), ((), ())), preferred_element_type=jnp.float32)
    dq_ref[...] = (dqt.T * scaling).astype(jnp.bfloat16)
    dk = jnp.dot(dsc, q, preferred_element_type=jnp.float32) * scaling
    dv = jnp.dot(pb, do, preferred_element_type=jnp.float32)
    for t in range(TOPK):
        a = dk[t * BLK : (t + 1) * BLK]
        b = dv[t * BLK : (t + 1) * BLK]
        mine_ref[names[t]] += jnp.where(first, a, b)
        other[names[t]] += jnp.where(first, b, a)

    @pl.when(i == pl.num_programs(0) - 1)
    def _():
        theirs_ref[...] = other[...].astype(jnp.bfloat16)


def reduce_kernel(
    n, mine, theirs, out_k, out_v, peer, got_down, got_up, put_down, put_up, final,
    ds, dr, us, ur, ps, pr, fs, fr,
):
    me, core, up, down, partner = places(n)
    rows = mine.shape[1]
    part = rows // SUB
    n_down = n // 2
    n_up = n - 1 - n_down
    greet((up, down, partner))
    order = []
    for t in range(n_down):
        order.append(("d", t))
        if t < n_up:
            order.append(("u", t))
    order.append(("own", 0))
    hand = {}

    def run_of(kind, t):
        if kind == "d":
            return lax.rem(me - n_down + t + n, n)
        if kind == "u":
            return lax.rem(me + n_up - t, n)
        return me

    for j, key in enumerate(order):
        run = run_of(*key)
        c = send(theirs.at[run], peer.at[run], ps.at[j], pr.at[j], partner)
        c.start()
        hand[key] = c
    started = []

    def base(run, u):
        s = pl.ds(u * part, part)
        return mine[run, s, :] + peer[run, s, :].astype(jnp.float32)

    def step(t, u, kind, put, got, s_sem, r_sem, where):
        run = run_of(kind, t)
        val = base(run, u)
        s = pl.ds(u * part, part)
        if t > 0:
            val = val + got[t - 1, s, :].astype(jnp.float32)
        put[t, s, :] = val.astype(jnp.bfloat16)
        c = send(put.at[t, s], got.at[t, s], s_sem.at[t * SUB + u], r_sem.at[t * SUB + u], where)
        c.start()
        started.append(c)
        return c

    downs = ups = None
    for t in range(n_down):
        next_downs, next_ups = [], []
        hand[("d", t)].wait_recv()
        if t < n_up:
            hand[("u", t)].wait_recv()
        for u in range(SUB):
            if t > 0:
                downs[u].wait_recv()
            next_downs.append(step(t, u, "d", put_down, got_down, ds, dr, down))
            if t < n_up:
                if t > 0:
                    ups[u].wait_recv()
                next_ups.append(step(t, u, "u", put_up, got_up, us, ur, up))
        if t == n_up:
            last_ups = ups
        downs, ups = next_downs, next_ups
    hand[("own", 0)].wait_recv()
    finals = []
    for u in range(SUB):
        s = pl.ds(u * part, part)
        last_ups[u].wait_recv()
        downs[u].wait_recv()
        val = base(me, u) + got_down[n_down - 1, s, :].astype(jnp.float32)
        val = (val + got_up[n_up - 1, s, :].astype(jnp.float32)).astype(jnp.bfloat16)
        final[core, s, :] = val
        c = send(final.at[core, s], final.at[core, s], fs.at[u], fr.at[u], partner)
        c.start()
        finals.append(c)
    for c in finals:
        c.wait_recv()
    for c in list(hand.values()) + started + finals:
        c.wait_send()
    out_k[...] = final[0]
    out_v[...] = final[1]


def vmem():
    return pl.BlockSpec(memory_space=pltpu.VMEM)


def anywhere():
    return pl.BlockSpec(memory_space=pl.ANY)


def per_device(queries, grad_out, keys, values, indices, valid):
    tokens, _, heads_here, width = queries.shape
    n = lax.axis_size("seq")
    seq_here = lax.axis_index("seq")
    blocks = tokens // BLK
    total_blocks = n * blocks
    scaling = 1.0 / math.sqrt(width)
    rows = BLK * heads_here
    half = n // 2
    rest = n - 1 - half
    dma = pltpu.SemaphoreType.DMA
    bf16, f32 = jnp.bfloat16, jnp.float32
    picks = lax.dynamic_slice_in_dim(indices[0], seq_here * blocks, blocks, 0)
    usable = lax.dynamic_slice_in_dim(valid[0], seq_here * blocks, blocks, 0)

    kv = pl.pallas_call(
        functools.partial(gather_kernel, n),
        out_shape=jax.ShapeDtypeStruct((2, n, tokens, width), bf16),
        in_specs=[anywhere()] * 2,
        out_specs=vmem(),
        scratch_shapes=[
            dma((2,)),
            dma((half * SUB,)), dma((half * SUB,)),
            dma((rest * SUB,)), dma((rest * SUB,)),
            dma((2 * half,)), dma((2 * half,)),
        ],
        compiler_params=pltpu.CompilerParams(collective_id=1, has_side_effects=True),
    )(keys[:, 0], values[:, 0])

    q2 = queries.reshape(tokens * heads_here, width)
    do2 = grad_out.reshape(tokens * heads_here, width)
    whole = lambda i, *_: (0, 0, 0)
    dq, mine, theirs = pl.pallas_call(
        functools.partial(attend_kernel, scaling),
        out_shape=(
            jax.ShapeDtypeStruct((tokens * heads_here, width), bf16),
            jax.ShapeDtypeStruct((total_blocks, BLK, width), f32),
            jax.ShapeDtypeStruct((total_blocks, BLK, width), bf16),
        ),
        grid_spec=pltpu.PrefetchScalarGridSpec(
            num_scalar_prefetch=2,
            grid=(blocks,),
            in_specs=[
                pl.BlockSpec((rows, width), lambda i, *_: (i, 0)),
                pl.BlockSpec((rows, width), lambda i, *_: (i, 0)),
                pl.BlockSpec((2, total_blocks, BLK, width), lambda i, *_: (0, 0, 0, 0)),
            ],
            out_specs=[
                pl.BlockSpec((rows, width), lambda i, *_: (i, 0)),
                pl.BlockSpec((total_blocks, BLK, width), whole),
                pl.BlockSpec((total_blocks, BLK, width), whole),
            ],
            scratch_shapes=[pltpu.VMEM((total_blocks, BLK, width), f32)],
        ),
        compiler_params=pltpu.CompilerParams(
            dimension_semantics=("arbitrary",), vmem_limit_bytes=60 * 2**20
        ),
    )(picks, usable, q2, do2, kv.reshape(2, total_blocks, BLK, width))

    gk, gv = pl.pallas_call(
        functools.partial(reduce_kernel, n),
        out_shape=(jax.ShapeDtypeStruct((tokens, width), bf16),) * 2,
        in_specs=[vmem()] * 2,
        out_specs=(vmem(), vmem()),
        scratch_shapes=[
            pltpu.VMEM((n, tokens, width), bf16),
            pltpu.VMEM((half, tokens, width), bf16),
            pltpu.VMEM((rest, tokens, width), bf16),
            pltpu.VMEM((half, tokens, width), bf16),
            pltpu.VMEM((rest, tokens, width), bf16),
            pltpu.VMEM((2, tokens, width), bf16),
            dma((half * SUB,)), dma((half * SUB,)),
            dma((rest * SUB,)), dma((rest * SUB,)),
            dma((n,)), dma((n,)),
            dma((SUB,)), dma((SUB,)),
        ],
        compiler_params=pltpu.CompilerParams(
            collective_id=2, has_side_effects=True, vmem_limit_bytes=60 * 2**20
        ),
    )(mine.reshape(n, tokens, width), theirs.reshape(n, tokens, width))
    return (
        dq.reshape(tokens, 1, heads_here, width),
        gk.reshape(tokens, 1, width),
        gv.reshape(tokens, 1, width),
    )


def solution(mesh):
    return jax.shard_map(
        per_device,
        mesh=mesh,
        in_specs=(
            P(("groups", "seq"), "head", "inner", None),
            P(("groups", "seq"), "head", "inner", None),
            P(("groups", "seq"), "head", None),
            P(("groups", "seq"), "head", None),
            P("head", "groups", None),
            P("head", "groups", None),
        ),
        out_specs=(
            P(("groups", "seq"), "head", "inner", None),
            P(("groups", "seq"), "head", None),
            P(("groups", "seq"), "head", None),
        ),
        check_vma=False,
    )
```

```python
import functools
import math

import jax
import jax.numpy as jnp
from jax import lax
from jax.experimental import pallas as pl
from jax.experimental.pallas import tpu as pltpu
from jax.sharding import PartitionSpec as P

BLK = 64
TOPK = 16
SUB = 4
MESH = pl.DeviceIdType.MESH
LOG2E = 1.4426950408889634


def places(n):
    me = lax.axis_index("seq")
    core = lax.axis_index("inner")
    up = {"seq": lax.rem(me + 1, n)}
    down = {"seq": lax.rem(me + n - 1, n)}
    partner = {"inner": 1 - core}
    return me, core, up, down, partner


def greet(n, me, up, down, partner):
    barrier = pltpu.get_barrier_semaphore()
    pl.semaphore_signal(barrier, inc=1, device_id=down, device_id_type=MESH)
    pl.semaphore_signal(barrier, inc=1, device_id=partner, device_id_type=MESH)

    @pl.when(me < n - 1)
    def _():
        pl.semaphore_signal(barrier, inc=1, device_id=up, device_id_type=MESH)

    pl.semaphore_wait(barrier, jnp.where(me > 0, 3, 2))


def send(src, dst, s_sem, r_sem, where):
    return pltpu.make_async_remote_copy(
        src_ref=src, dst_ref=dst, send_sem=s_sem, recv_sem=r_sem, device_id=where, device_id_type=MESH
    )


def gather_kernel(n, k_ref, v_ref, kv_ref, local_sem, us, ur, ws, wr, ps, pr, ready):
    me, core, up, down, partner = places(n)
    rows = k_ref.shape[0]
    part = rows // SUB
    half = n // 2
    wraps = n - 1 - half
    last = n - 1
    own_k = pltpu.make_async_copy(k_ref, kv_ref.at[0, me], local_sem.at[0])
    own_v = pltpu.make_async_copy(v_ref, kv_ref.at[1, me], local_sem.at[1])
    own_k.start()
    own_v.start()
    greet(n, me, up, down, partner)

    @pl.when(me == last)
    def _():
        pl.semaphore_signal(ready, inc=1, device_id=up, device_id_type=MESH)

    own_k.wait()
    own_v.wait()

    def piece(run, u):
        return kv_ref.at[core, run, pl.ds(u * part, part)]

    def up_copy(run, u):
        return send(piece(run, u), piece(run, u), us.at[run, u], ur.at[run, u], up)

    def wrap_copy(run, u):
        return send(piece(run, u), piece(run, u), ws.at[run, u], wr.at[run, u], down)

    def share_copy(run):
        return send(kv_ref.at[core, run], kv_ref.at[core, run], ps.at[run], pr.at[run], partner)

    @pl.when(me < last)
    def _():
        for u in range(SUB):
            up_copy(me, u).start()

    @pl.when(me == 0)
    def _():
        pl.semaphore_wait(ready, 1)

    lag = jnp.where(me > half, (5 * (last - me) + 2) // 3, 0)
    for j in range(wraps + half - 2 + 2):
        if j < half:
            run = me - 1 - j

            @pl.when(run >= 0)
            def _():
                for u in range(SUB):
                    up_copy(run, u).wait_recv()
                    if j + 1 < half:

                        @pl.when(me < last)
                        def _():
                            up_copy(run, u).start()

                share_copy(run).start()

        w = j - lag
        low = (me <= w) & (w < wraps)

        @pl.when(low)
        def _():
            for u in range(SUB):

                @pl.when(w > me)
                def _():
                    wrap_copy(w, u).wait_recv()

                wrap_copy(w, u).start()

        @pl.when((w >= 0) & (w + half < me))
        def _():
            for u in range(SUB):
                wrap_copy(w, u).wait_recv()

                @pl.when(w + half + 1 < me)
                def _():
                    wrap_copy(w, u).start()

            share_copy(w).start()

    for run in range(n - 1):

        @pl.when(run < me)
        def _():
            share_copy(run).wait_recv()
            share_copy(run).wait_send()

        @pl.when((run <= me) & (me < min(run + half, last)))
        def _():
            for u in range(SUB):
                up_copy(run, u).wait_send()

        if run < wraps:

            @pl.when((me <= run) | (me > run + half + 1))
            def _():
                for u in range(SUB):
                    wrap_copy(run, u).wait_send()


def attend_kernel(scaling, picks, usable, q_ref, do_ref, kv_ref, dq_ref, tiles_ref, acc):
    i = pl.program_id(0)
    at = lax.axis_index("seq") * pl.num_programs(0) + i
    rows = q_ref.shape[0]
    per_pos = rows // BLK

    @pl.when(i == 0)
    def _():
        acc[...] = jnp.zeros_like(acc)

    q = q_ref[...]
    do = do_ref[...]
    names = [jnp.where(usable[t, at] > 0, picks[t, at], at) for t in range(TOPK)]
    ks = jnp.concatenate([kv_ref[0, b] for b in names], axis=0)
    vs = jnp.concatenate([kv_ref[1, b] for b in names], axis=0)
    nt = (((1,), (1,)), ((), ()))
    st = lax.dot_general(ks, q, nt, preferred_element_type=jnp.float32)
    key_at = lax.broadcasted_iota(jnp.int32, (BLK, rows), 0)
    query_at = lax.broadcasted_iota(jnp.int32, (BLK, rows), 1) // per_pos
    low = jnp.float32(-1e30)
    parts = [jnp.where(key_at <= query_at, st[:BLK], low)]
    for t in range(1, TOPK):
        bias = jnp.where(usable[t, at] > 0, jnp.float32(0.0), low)
        parts.append(st[t * BLK : (t + 1) * BLK] + bias)
    st = jnp.concatenate(parts, axis=0)
    top = jnp.max(st, axis=0, keepdims=True)
    w = jnp.exp2((st - top) * jnp.float32(scaling * LOG2E))
    inv = 1.0 / jnp.sum(w, axis=0, keepdims=True)
    p = w * inv
    dp = lax.dot_general(vs, do, nt, preferred_element_type=jnp.float32)
    delta = jnp.sum(p * dp, axis=0, keepdims=True)
    dsc = (p * (dp - delta)).astype(jnp.bfloat16)
    pb = p.astype(jnp.bfloat16)
    dqt = lax.dot_general(ks, dsc, (((0,), (0,)), ((), ())), preferred_element_type=jnp.float32)
    dq_ref[...] = (dqt.T * scaling).astype(jnp.bfloat16)
    dk = jnp.dot(dsc, q, preferred_element_type=jnp.float32) * scaling
    dv = jnp.dot(pb, do, preferred_element_type=jnp.float32)
    for t in range(TOPK):
        acc[0, names[t]] += dk[t * BLK : (t + 1) * BLK]
        acc[1, names[t]] += dv[t * BLK : (t + 1) * BLK]

    @pl.when(i == pl.num_programs(0) - 1)
    def _():
        tiles_ref[...] = acc[...].astype(jnp.bfloat16)


def reduce_kernel(
    n, tiles, out, peer, got_down, got_up, put_down, put_up, final, ds, dr, us, ur, ps, pr, fs, fr
):
    me, core, up, down, partner = places(n)
    rows = tiles.shape[2]
    part = rows // SUB
    half = n // 2
    wraps = n - 1 - half
    last = n - 1
    greet(n, me, up, down, partner)

    def hand(run):
        return send(tiles.at[1 - core, run], peer.at[run], ps.at[run], pr.at[run], partner)

    for t in range(half):
        for run in (me - half + t, me - half - 1 - t):

            @pl.when(run >= 0)
            def _():
                hand(run).start()

    hand(me).start()

    def base(run, u):
        s = pl.ds(u * part, part)
        return tiles[core, run, s, :].astype(jnp.float32) + peer[run, s, :].astype(jnp.float32)

    def down_copy(run, u):
        s = pl.ds(u * part, part)
        return send(put_down.at[run, s], got_down.at[run, s], ds.at[run, u], dr.at[run, u], down)

    def up_copy(run, u, put):
        s = pl.ds(u * part, part)
        return send(put.at[run, s], got_up.at[run, s], us.at[run, u], ur.at[run, u], up)

    for t in range(half):
        wrap = me - half - 1 - t
        run = me - half + t

        @pl.when(wrap >= 0)
        def _():
            hand(wrap).wait_recv()
            for u in range(SUB):
                s = pl.ds(u * part, part)
                val = base(wrap, u)
                if t > 0:
                    up_copy(wrap, u, put_up).wait_recv()
                    val = val + got_up[wrap, s, :].astype(jnp.float32)
                put_up[wrap, s, :] = val.astype(jnp.bfloat16)
                up_copy(wrap, u, put_up).start()

        @pl.when(run >= 0)
        def _():
            hand(run).wait_recv()
            for u in range(SUB):
                s = pl.ds(u * part, part)
                if t == 0:
                    put_down[run, s, :] = base(run, u).astype(jnp.bfloat16)
                else:

                    @pl.when(me < last)
                    def _():
                        down_copy(run, u).wait_recv()
                        val = base(run, u) + got_down[run, s, :].astype(jnp.float32)
                        put_down[run, s, :] = val.astype(jnp.bfloat16)

                    @pl.when(me == last)
                    def _():
                        put_down[run, s, :] = base(run, u).astype(jnp.bfloat16)

                down_copy(run, u).start()

    for o in range(wraps - 1, 0, -1):

        @pl.when(me < o)
        def _():
            for u in range(SUB):
                up_copy(o, u, got_up).wait_recv()
                up_copy(o, u, got_up).start()

    hand(me).wait_recv()
    for u in range(SUB):
        s = pl.ds(u * part, part)

        @pl.when(me < last)
        def _():
            down_copy(me, u).wait_recv()

        @pl.when(me < wraps)
        def _():
            up_copy(me, u, got_up).wait_recv()
            final[core, s, :] = (
                base(me, u)
                + got_down[me, s, :].astype(jnp.float32)
                + got_up[me, s, :].astype(jnp.float32)
            ).astype(jnp.bfloat16)

        @pl.when((me >= wraps) & (me < last))
        def _():
            val = base(me, u) + got_down[me, s, :].astype(jnp.float32)
            final[core, s, :] = val.astype(jnp.bfloat16)

        @pl.when(me == last)
        def _():
            final[core, s, :] = base(me, u).astype(jnp.bfloat16)

        send(final.at[core, s], final.at[core, s], fs.at[u], fr.at[u], partner).start()
    for u in range(SUB):
        s = pl.ds(u * part, part)
        send(final.at[core, s], final.at[core, s], fs.at[u], fr.at[u], partner).wait()
    for run in range(n):

        @pl.when(run <= me)
        def _():
            hand(run).wait_send()

        @pl.when((run < me) & (me <= run + half))
        def _():
            for u in range(SUB):
                down_copy(run, u).wait_send()

        if run < wraps:

            @pl.when((me < run) | (me > run + half))
            def _():
                for u in range(SUB):
                    up_copy(run, u, got_up).wait_send()

    out[...] = final[...]


def vmem():
    return pl.BlockSpec(memory_space=pltpu.VMEM)


def anywhere():
    return pl.BlockSpec(memory_space=pl.ANY)


def per_device(queries, grad_out, keys, values, indices, valid):
    tokens, _, heads_here, width = queries.shape
    n = lax.axis_size("seq")
    blocks = tokens // BLK
    total_blocks = n * blocks
    scaling = 1.0 / math.sqrt(width)
    rows = BLK * heads_here
    half = n // 2
    rest = n - 1 - half
    dma = pltpu.SemaphoreType.DMA
    bf16, f32 = jnp.bfloat16, jnp.float32
    picks, usable = indices[0].T, valid[0].T

    kv = pl.pallas_call(
        functools.partial(gather_kernel, n),
        out_shape=jax.ShapeDtypeStruct((2, n, tokens, width), bf16),
        in_specs=[anywhere()] * 2,
        out_specs=vmem(),
        scratch_shapes=[
            dma((2,)),
            dma((n, SUB)), dma((n, SUB)),
            dma((rest, SUB)), dma((rest, SUB)),
            dma((n,)), dma((n,)),
            pltpu.SemaphoreType.REGULAR,
        ],
        compiler_params=pltpu.CompilerParams(collective_id=1, has_side_effects=True),
    )(keys[:, 0], values[:, 0])

    q2 = queries.reshape(tokens * heads_here, width)
    do2 = grad_out.reshape(tokens * heads_here, width)
    full = (2, total_blocks, BLK, width)
    whole = lambda i, *_: (0, 0, 0, 0)
    by_block = pl.BlockSpec((rows, width), lambda i, *_: (i, 0))
    dq, tiles = pl.pallas_call(
        functools.partial(attend_kernel, scaling),
        out_shape=(
            jax.ShapeDtypeStruct((tokens * heads_here, width), bf16),
            jax.ShapeDtypeStruct(full, bf16),
        ),
        grid_spec=pltpu.PrefetchScalarGridSpec(
            num_scalar_prefetch=2,
            grid=(blocks,),
            in_specs=[by_block, by_block, pl.BlockSpec(full, whole)],
            out_specs=[by_block, pl.BlockSpec(full, whole)],
            scratch_shapes=[pltpu.VMEM(full, f32)],
        ),
        compiler_params=pltpu.CompilerParams(
            dimension_semantics=("arbitrary",), vmem_limit_bytes=60 * 2**20
        ),
    )(picks, usable, q2, do2, kv.reshape(full))

    own = pl.pallas_call(
        functools.partial(reduce_kernel, n),
        out_shape=jax.ShapeDtypeStruct((2, tokens, width), bf16),
        in_specs=[vmem()],
        out_specs=vmem(),
        scratch_shapes=[
            pltpu.VMEM((n, tokens, width), bf16),
            pltpu.VMEM((n, tokens, width), bf16),
            pltpu.VMEM((rest, tokens, width), bf16),
            pltpu.VMEM((n, tokens, width), bf16),
            pltpu.VMEM((rest, tokens, width), bf16),
            pltpu.VMEM((2, tokens, width), bf16),
            dma((n, SUB)), dma((n, SUB)),
            dma((rest, SUB)), dma((rest, SUB)),
            dma((n,)), dma((n,)),
            dma((SUB,)), dma((SUB,)),
        ],
        compiler_params=pltpu.CompilerParams(
            collective_id=2, has_side_effects=True, vmem_limit_bytes=60 * 2**20
        ),
    )(tiles.reshape(2, n, tokens, width))
    gk, gv = own[0], own[1]
    return (
        dq.reshape(tokens, 1, heads_here, width),
        gk.reshape(tokens, 1, width),
        gv.reshape(tokens, 1, width),
    )


def solution(mesh):
    return jax.shard_map(
        per_device,
        mesh=mesh,
        in_specs=(
            P(("groups", "seq"), "head", "inner", None),
            P(("groups", "seq"), "head", "inner", None),
            P(("groups", "seq"), "head", None),
            P(("groups", "seq"), "head", None),
            P("head", "groups", None),
            P("head", "groups", None),
        ),
        out_specs=(
            P(("groups", "seq"), "head", "inner", None),
            P(("groups", "seq"), "head", None),
            P(("groups", "seq"), "head", None),
        ),
        check_vma=False,
    )
```

```python
import functools
import math

import jax
import jax.numpy as jnp
from jax import lax
from jax.experimental import pallas as pl
from jax.experimental.pallas import tpu as pltpu
from jax.sharding import PartitionSpec as P

BLK = 64
TOPK = 16
SUB = 4
MESH = pl.DeviceIdType.MESH
LOG2E = 1.4426950408889634


def places(n):
    me = lax.axis_index("seq")
    core = lax.axis_index("inner")
    up = {"seq": lax.rem(me + 1, n)}
    down = {"seq": lax.rem(me + n - 1, n)}
    partner = {"inner": 1 - core}
    return me, core, up, down, partner


def meet(signals, count):
    barrier = pltpu.get_barrier_semaphore()
    for needed, where in signals:

        @pl.when(needed)
        def _():
            pl.semaphore_signal(barrier, inc=1, device_id=where, device_id_type=MESH)

    pl.semaphore_wait(barrier, count)


def one_if(cond):
    return jnp.where(cond, 1, 0)


def send(src, dst, s_sem, r_sem, where):
    return pltpu.make_async_remote_copy(
        src_ref=src, dst_ref=dst, send_sem=s_sem, recv_sem=r_sem, device_id=where, device_id_type=MESH
    )


def gather_kernel(n, k_ref, v_ref, kv_ref, local_sem, us, ur, ws, wr, ps, pr, ready):
    me, core, up, down, partner = places(n)
    rows = k_ref.shape[0]
    part = rows // SUB
    half = n // 2
    wraps = n - 1 - half
    last = n - 1
    own_k = pltpu.make_async_copy(k_ref, kv_ref.at[0, me], local_sem.at[0])
    own_v = pltpu.make_async_copy(v_ref, kv_ref.at[1, me], local_sem.at[1])
    own_k.start()
    own_v.start()
    far = {"seq": last}
    meet(
        (
            (me > 0, partner),
            (me > 0, down),
            ((me > half) & (me < last), up),
            (me < wraps, far),
        ),
        one_if(me > 0) + one_if(me < last) + one_if(me > half + 1) + jnp.where(me == last, wraps, 0),
    )

    @pl.when(me == last)
    def _():
        for s in range(wraps):
            pl.semaphore_signal(ready, inc=1, device_id={"seq": s}, device_id_type=MESH)

    own_k.wait()
    own_v.wait()

    def piece(run, u):
        return kv_ref.at[core, run, pl.ds(u * part, part)]

    def up_copy(run, u):
        return send(piece(run, u), piece(run, u), us.at[run, u], ur.at[run, u], up)

    def wrap_copy(run, u):
        return send(piece(run, u), piece(run, u), ws.at[run, u], wr.at[run, u], down)

    def share_copy(run):
        return send(kv_ref.at[core, run], kv_ref.at[core, run], ps.at[run], pr.at[run], partner)

    @pl.when(me < last)
    def _():
        for u in range(SUB):
            up_copy(me, u).start()

    def own_wrap():
        pl.semaphore_wait(ready, 1)
        for u in range(SUB):
            send(piece(me, u), piece(me, u), ws.at[me, u], wr.at[me, u], far).start()

    @pl.when(me == 0)
    def _():
        own_wrap()

    lag = (5 * (last - me) + 2) // 3
    for j in range(wraps + half - 2):
        if j < half:
            run = me - 1 - j

            @pl.when((run == 0) & (me > half // 2) & (me < wraps))
            def _():
                own_wrap()

            @pl.when(run >= 0)
            def _():
                for u in range(SUB):
                    up_copy(run, u).wait_recv()
                    if j + 1 < half:

                        @pl.when(me < last)
                        def _():
                            up_copy(run, u).start()

                share_copy(run).start()

            @pl.when((run == 0) & (me <= half // 2))
            def _():
                own_wrap()

        w = j - lag
        @pl.when((w >= 0) & (w + half < me))
        def _():
            for u in range(SUB):
                wrap_copy(w, u).wait_recv()

                @pl.when(w + half + 1 < me)
                def _():
                    wrap_copy(w, u).start()

            share_copy(w).start()

    for run in range(n - 1):

        @pl.when(run < me)
        def _():
            share_copy(run).wait_recv()
            share_copy(run).wait_send()

        @pl.when((run <= me) & (me < min(run + half, last)))
        def _():
            for u in range(SUB):
                up_copy(run, u).wait_send()

        if run < wraps:

            @pl.when((me == run) | (me > run + half + 1))
            def _():
                for u in range(SUB):
                    wrap_copy(run, u).wait_send()


def attend_kernel(scaling, picks, usable, q_ref, do_ref, kv_ref, dq_ref, tiles_ref, acc):
    i = pl.program_id(0)
    at = lax.axis_index("seq") * pl.num_programs(0) + i
    rows = q_ref.shape[0]
    per_pos = rows // BLK

    @pl.when(i == 0)
    def _():
        acc[...] = jnp.zeros_like(acc)

    q = q_ref[...]
    do = do_ref[...]
    names = [jnp.where(usable[t, at] > 0, picks[t, at], at) for t in range(TOPK)]
    ks = jnp.concatenate([kv_ref[0, b] for b in names], axis=0)
    vs = jnp.concatenate([kv_ref[1, b] for b in names], axis=0)
    nt = (((1,), (1,)), ((), ()))
    st = lax.dot_general(ks, q, nt, preferred_element_type=jnp.float32)
    key_at = lax.broadcasted_iota(jnp.int32, (BLK, rows), 0)
    query_at = lax.broadcasted_iota(jnp.int32, (BLK, rows), 1) // per_pos
    low = jnp.float32(-1e30)
    parts = [jnp.where(key_at <= query_at, st[:BLK], low)]
    for t in range(1, TOPK):
        bias = jnp.where(usable[t, at] > 0, jnp.float32(0.0), low)
        parts.append(st[t * BLK : (t + 1) * BLK] + bias)
    st = jnp.concatenate(parts, axis=0)
    top = jnp.max(st, axis=0, keepdims=True)
    w = jnp.exp2((st - top) * jnp.float32(scaling * LOG2E))
    inv = 1.0 / jnp.sum(w, axis=0, keepdims=True)
    p = w * inv
    dp = lax.dot_general(vs, do, nt, preferred_element_type=jnp.float32)
    delta = jnp.sum(p * dp, axis=0, keepdims=True)
    dsc = (p * (dp - delta)).astype(jnp.bfloat16)
    pb = p.astype(jnp.bfloat16)
    dqt = lax.dot_general(ks, dsc, (((0,), (0,)), ((), ())), preferred_element_type=jnp.float32)
    dq_ref[...] = (dqt.T * scaling).astype(jnp.bfloat16)
    dk = jnp.dot(dsc, q, preferred_element_type=jnp.float32) * scaling
    dv = jnp.dot(pb, do, preferred_element_type=jnp.float32)
    for t in range(TOPK):
        acc[0, names[t]] += dk[t * BLK : (t + 1) * BLK]
        acc[1, names[t]] += dv[t * BLK : (t + 1) * BLK]

    @pl.when(i == pl.num_programs(0) - 1)
    def _():
        tiles_ref[...] = acc[...].astype(jnp.bfloat16)


def reduce_kernel(
    n, tiles, out, peer, got_down, got_up, put_down, put_up, final, ds, dr, us, ur, ps, pr, fs, fr
):
    me, core, up, down, partner = places(n)
    rows = tiles.shape[2]
    part = rows // SUB
    half = n // 2
    wraps = n - 1 - half
    last = n - 1
    far = {"seq": last}
    meet(
        (
            (me >= 0, partner),
            (me < last, up),
            (me > half + 1, down),
            (me < wraps, far),
        ),
        1 + one_if(me > 0) + one_if((me > half) & (me < last)) + jnp.where(me == last, wraps, 0),
    )

    def hand(run):
        return send(tiles.at[1 - core, run], peer.at[run], ps.at[run], pr.at[run], partner)

    for t in range(half):
        for run in (me - half + t, me - half - 1 - t):

            @pl.when(run >= 0)
            def _():
                hand(run).start()

    hand(me).start()

    def base(run, u):
        s = pl.ds(u * part, part)
        return tiles[core, run, s, :].astype(jnp.float32) + peer[run, s, :].astype(jnp.float32)

    def down_copy(run, u):
        s = pl.ds(u * part, part)
        return send(put_down.at[run, s], got_down.at[run, s], ds.at[run, u], dr.at[run, u], down)

    def up_copy(run, u):
        s = pl.ds(u * part, part)
        where = {"seq": jnp.where(me == last, run, lax.rem(me + 1, n))}
        return send(put_up.at[run, s], got_up.at[run, s], us.at[run, u], ur.at[run, u], where)

    for t in range(half):
        wrap = me - half - 1 - t
        run = me - half + t

        @pl.when(wrap >= 0)
        def _():
            hand(wrap).wait_recv()
            for u in range(SUB):
                s = pl.ds(u * part, part)
                val = base(wrap, u)
                if t > 0:
                    up_copy(wrap, u).wait_recv()
                    val = val + got_up[wrap, s, :].astype(jnp.float32)
                put_up[wrap, s, :] = val.astype(jnp.bfloat16)
                up_copy(wrap, u).start()

        @pl.when(run >= 0)
        def _():
            hand(run).wait_recv()
            for u in range(SUB):
                s = pl.ds(u * part, part)
                if t == 0:
                    put_down[run, s, :] = base(run, u).astype(jnp.bfloat16)
                else:

                    @pl.when(me < last)
                    def _():
                        down_copy(run, u).wait_recv()
                        val = base(run, u) + got_down[run, s, :].astype(jnp.float32)
                        put_down[run, s, :] = val.astype(jnp.bfloat16)

                    @pl.when(me == last)
                    def _():
                        put_down[run, s, :] = base(run, u).astype(jnp.bfloat16)

                down_copy(run, u).start()

    hand(me).wait_recv()
    for u in range(SUB):
        s = pl.ds(u * part, part)

        @pl.when(me < last)
        def _():
            down_copy(me, u).wait_recv()

        @pl.when(me < wraps)
        def _():
            up_copy(me, u).wait_recv()
            final[core, s, :] = (
                base(me, u)
                + got_down[me, s, :].astype(jnp.float32)
                + got_up[me, s, :].astype(jnp.float32)
            ).astype(jnp.bfloat16)

        @pl.when((me >= wraps) & (me < last))
        def _():
            val = base(me, u) + got_down[me, s, :].astype(jnp.float32)
            final[core, s, :] = val.astype(jnp.bfloat16)

        @pl.when(me == last)
        def _():
            final[core, s, :] = base(me, u).astype(jnp.bfloat16)

        send(final.at[core, s], final.at[core, s], fs.at[u], fr.at[u], partner).start()
    for u in range(SUB):
        s = pl.ds(u * part, part)
        send(final.at[core, s], final.at[core, s], fs.at[u], fr.at[u], partner).wait()
    for run in range(n):

        @pl.when(run <= me)
        def _():
            hand(run).wait_send()

        @pl.when((run < me) & (me <= run + half))
        def _():
            for u in range(SUB):
                down_copy(run, u).wait_send()

        if run < wraps:

            @pl.when(me > run + half)
            def _():
                for u in range(SUB):
                    up_copy(run, u).wait_send()

    out[...] = final[...]


def vmem():
    return pl.BlockSpec(memory_space=pltpu.VMEM)


def anywhere():
    return pl.BlockSpec(memory_space=pl.ANY)


def per_device(queries, grad_out, keys, values, indices, valid):
    tokens, _, heads_here, width = queries.shape
    n = lax.axis_size("seq")
    blocks = tokens // BLK
    total_blocks = n * blocks
    scaling = 1.0 / math.sqrt(width)
    rows = BLK * heads_here
    half = n // 2
    rest = n - 1 - half
    dma = pltpu.SemaphoreType.DMA
    bf16, f32 = jnp.bfloat16, jnp.float32
    picks, usable = indices[0].T, valid[0].T

    kv = pl.pallas_call(
        functools.partial(gather_kernel, n),
        out_shape=jax.ShapeDtypeStruct((2, n, tokens, width), bf16),
        in_specs=[anywhere()] * 2,
        out_specs=vmem(),
        scratch_shapes=[
            dma((2,)),
            dma((n, SUB)), dma((n, SUB)),
            dma((rest, SUB)), dma((rest, SUB)),
            dma((n,)), dma((n,)),
            pltpu.SemaphoreType.REGULAR,
        ],
        compiler_params=pltpu.CompilerParams(collective_id=1, has_side_effects=True),
    )(keys[:, 0], values[:, 0])

    q2 = queries.reshape(tokens * heads_here, width)
    do2 = grad_out.reshape(tokens * heads_here, width)
    full = (2, total_blocks, BLK, width)
    whole = lambda i, *_: (0, 0, 0, 0)
    by_block = pl.BlockSpec((rows, width), lambda i, *_: (i, 0))
    dq, tiles = pl.pallas_call(
        functools.partial(attend_kernel, scaling),
        out_shape=(
            jax.ShapeDtypeStruct((tokens * heads_here, width), bf16),
            jax.ShapeDtypeStruct(full, bf16),
        ),
        grid_spec=pltpu.PrefetchScalarGridSpec(
            num_scalar_prefetch=2,
            grid=(blocks,),
            in_specs=[by_block, by_block, pl.BlockSpec(full, whole)],
            out_specs=[by_block, pl.BlockSpec(full, whole)],
            scratch_shapes=[pltpu.VMEM(full, f32)],
        ),
        compiler_params=pltpu.CompilerParams(
            dimension_semantics=("arbitrary",), vmem_limit_bytes=60 * 2**20
        ),
    )(picks, usable, q2, do2, kv.reshape(full))

    own = pl.pallas_call(
        functools.partial(reduce_kernel, n),
        out_shape=jax.ShapeDtypeStruct((2, tokens, width), bf16),
        in_specs=[vmem()],
        out_specs=vmem(),
        scratch_shapes=[
            pltpu.VMEM((n, tokens, width), bf16),
            pltpu.VMEM((n, tokens, width), bf16),
            pltpu.VMEM((rest, tokens, width), bf16),
            pltpu.VMEM((n, tokens, width), bf16),
            pltpu.VMEM((rest, tokens, width), bf16),
            pltpu.VMEM((2, tokens, width), bf16),
            dma((n, SUB)), dma((n, SUB)),
            dma((rest, SUB)), dma((rest, SUB)),
            dma((n,)), dma((n,)),
            dma((SUB,)), dma((SUB,)),
        ],
        compiler_params=pltpu.CompilerParams(
            collective_id=2, has_side_effects=True, vmem_limit_bytes=60 * 2**20
        ),
    )(tiles.reshape(2, n, tokens, width))
    gk, gv = own[0], own[1]
    return (
        dq.reshape(tokens, 1, heads_here, width),
        gk.reshape(tokens, 1, width),
        gv.reshape(tokens, 1, width),
    )


def solution(mesh):
    return jax.shard_map(
        per_device,
        mesh=mesh,
        in_specs=(
            P(("groups", "seq"), "head", "inner", None),
            P(("groups", "seq"), "head", "inner", None),
            P(("groups", "seq"), "head", None),
            P(("groups", "seq"), "head", None),
            P("head", "groups", None),
            P("head", "groups", None),
        ),
        out_specs=(
            P(("groups", "seq"), "head", "inner", None),
            P(("groups", "seq"), "head", None),
            P(("groups", "seq"), "head", None),
        ),
        check_vma=False,
    )
```

```python
import functools
import math

import jax
import jax.numpy as jnp
from jax import lax
from jax.experimental import pallas as pl
from jax.experimental.pallas import tpu as pltpu
from jax.sharding import PartitionSpec as P

BLK = 64
TOPK = 16
SUB = 4
MESH = pl.DeviceIdType.MESH
LOG2E = 1.4426950408889634


def places(n):
    me = lax.axis_index("seq")
    core = lax.axis_index("inner")
    up = {"seq": lax.rem(me + 1, n)}
    down = {"seq": lax.rem(me + n - 1, n)}
    partner = {"inner": 1 - core}
    return me, core, up, down, partner


def greet(n, me, up, down, partner):
    barrier = pltpu.get_barrier_semaphore()
    pl.semaphore_signal(barrier, inc=1, device_id=down, device_id_type=MESH)
    pl.semaphore_signal(barrier, inc=1, device_id=partner, device_id_type=MESH)

    @pl.when(me < n - 1)
    def _():
        pl.semaphore_signal(barrier, inc=1, device_id=up, device_id_type=MESH)

    pl.semaphore_wait(barrier, jnp.where(me > 0, 3, 2))


def send(src, dst, s_sem, r_sem, where):
    return pltpu.make_async_remote_copy(
        src_ref=src, dst_ref=dst, send_sem=s_sem, recv_sem=r_sem, device_id=where, device_id_type=MESH
    )


def gather_kernel(n, k_ref, v_ref, kv_ref, local_sem, us, ur, ws, wr, ps, pr, ready):
    me, core, up, down, partner = places(n)
    rows = k_ref.shape[0]
    part = rows // SUB
    half = n // 2
    wraps = n - 1 - half
    last = n - 1
    own_k = pltpu.make_async_copy(k_ref, kv_ref.at[0, me], local_sem.at[0])
    own_v = pltpu.make_async_copy(v_ref, kv_ref.at[1, me], local_sem.at[1])
    own_k.start()
    own_v.start()
    greet(n, me, up, down, partner)

    @pl.when(me == last)
    def _():
        pl.semaphore_signal(ready, inc=1, device_id=up, device_id_type=MESH)

    own_k.wait()
    own_v.wait()

    def piece(run, u):
        return kv_ref.at[core, run, pl.ds(u * part, part)]

    def up_copy(run, u):
        return send(piece(run, u), piece(run, u), us.at[run, u], ur.at[run, u], up)

    def wrap_copy(run, u):
        return send(piece(run, u), piece(run, u), ws.at[run, u], wr.at[run, u], down)

    def share_copy(run):
        return send(kv_ref.at[core, run], kv_ref.at[core, run], ps.at[run], pr.at[run], partner)

    @pl.when(me < last)
    def _():
        for u in range(SUB):
            up_copy(me, u).start()

    def pass_on(w):
        for u in range(SUB):

            @pl.when(w > me)
            def _():
                wrap_copy(w, u).wait_recv()

            wrap_copy(w, u).start()

    @pl.when(me == 0)
    def _():
        pl.semaphore_wait(ready, 1)

    for w in range(wraps):

        @pl.when((me == 0) | (me == w))
        def _():
            pass_on(w)

    lag = (5 * (last - me) + 2) // 3
    for j in range(wraps + half - 2 + 2):
        if j < half:
            run = me - 1 - j

            @pl.when(run == 0)
            def _():
                for w in range(1, wraps):

                    @pl.when(w > me)
                    def _():
                        pass_on(w)

            @pl.when(run >= 0)
            def _():
                for u in range(SUB):
                    up_copy(run, u).wait_recv()
                    if j + 1 < half:

                        @pl.when(me < last)
                        def _():
                            up_copy(run, u).start()

                share_copy(run).start()

        w = j - lag
        @pl.when((w >= 0) & (w + half < me))
        def _():
            for u in range(SUB):
                wrap_copy(w, u).wait_recv()

                @pl.when(w + half + 1 < me)
                def _():
                    wrap_copy(w, u).start()

            share_copy(w).start()

    for run in range(n - 1):

        @pl.when(run < me)
        def _():
            share_copy(run).wait_recv()
            share_copy(run).wait_send()

        @pl.when((run <= me) & (me < min(run + half, last)))
        def _():
            for u in range(SUB):
                up_copy(run, u).wait_send()

        if run < wraps:

            @pl.when((me <= run) | (me > run + half + 1))
            def _():
                for u in range(SUB):
                    wrap_copy(run, u).wait_send()


def attend_kernel(
    scaling, n, picks, usable, q_ref, do_ref, kv_hbm, dq_ref, tiles_ref, acc, kv_ref, stage, in_sem, out_sem
):
    i = pl.program_id(0)
    at = lax.axis_index("seq") * pl.num_programs(0) + i
    rows = q_ref.shape[0]
    per_pos = rows // BLK

    @pl.when(i == 0)
    def _():
        load = pltpu.make_async_copy(kv_hbm, kv_ref, in_sem)
        load.start()
        acc[...] = jnp.zeros_like(acc)
        load.wait()

    q = q_ref[...]
    do = do_ref[...]
    names = [jnp.where(usable[t, at] > 0, picks[t, at], at) for t in range(TOPK)]
    ks = jnp.concatenate([kv_ref[0, b] for b in names], axis=0)
    vs = jnp.concatenate([kv_ref[1, b] for b in names], axis=0)
    nt = (((1,), (1,)), ((), ()))
    st = lax.dot_general(ks, q, nt, preferred_element_type=jnp.float32)
    key_at = lax.broadcasted_iota(jnp.int32, (BLK, rows), 0)
    query_at = lax.broadcasted_iota(jnp.int32, (BLK, rows), 1) // per_pos
    low = jnp.float32(-1e30)
    parts = [jnp.where(key_at <= query_at, st[:BLK], low)]
    for t in range(1, TOPK):
        bias = jnp.where(usable[t, at] > 0, jnp.float32(0.0), low)
        parts.append(st[t * BLK : (t + 1) * BLK] + bias)
    st = jnp.concatenate(parts, axis=0)
    top = jnp.max(st, axis=0, keepdims=True)
    w = jnp.exp2((st - top) * jnp.float32(scaling * LOG2E))
    inv = 1.0 / jnp.sum(w, axis=0, keepdims=True)
    p = w * inv
    dp = lax.dot_general(vs, do, nt, preferred_element_type=jnp.float32)
    delta = jnp.sum(p * dp, axis=0, keepdims=True)
    dsc = (p * (dp - delta)).astype(jnp.bfloat16)
    pb = p.astype(jnp.bfloat16)
    dqt = lax.dot_general(ks, dsc, (((0,), (0,)), ((), ())), preferred_element_type=jnp.float32)
    dq_ref[...] = (dqt.T * scaling).astype(jnp.bfloat16)
    dk = jnp.dot(dsc, q, preferred_element_type=jnp.float32) * scaling
    dv = jnp.dot(pb, do, preferred_element_type=jnp.float32)
    for t in range(TOPK):
        acc[0, names[t]] += dk[t * BLK : (t + 1) * BLK]
        acc[1, names[t]] += dv[t * BLK : (t + 1) * BLK]

    @pl.when(i == pl.num_programs(0) - 1)
    def _():
        per_run = acc.shape[1] // n
        outs = []
        for r in range(n):
            s = pl.ds(r * per_run, per_run)
            stage[:, s] = acc[:, s].astype(jnp.bfloat16)
            c = pltpu.make_async_copy(stage.at[:, s], tiles_ref.at[:, s], out_sem.at[r])
            c.start()
            outs.append(c)
        for c in outs:
            c.wait()


def reduce_kernel(
    n, tiles_hbm, out, tiles, ls, peer, got_down, got_up, put_down, put_up, final, ds, dr, us, ur, ps, pr, fs, fr
):
    me, core, up, down, partner = places(n)
    rows = tiles.shape[2]
    part = rows // SUB
    half = n // 2
    wraps = n - 1 - half
    last = n - 1

    def load(run):
        return pltpu.make_async_copy(tiles_hbm.at[:, run], tiles.at[:, run], ls.at[run])

    for t in range(half):
        for run in (me - half - 1 - t, me - half + t):

            @pl.when(run >= 0)
            def _():
                load(run).start()

    load(me).start()
    greet(n, me, up, down, partner)

    def hand(run):
        return send(tiles.at[1 - core, run], peer.at[run], ps.at[run], pr.at[run], partner)

    for t in range(half):
        for run in (me - half - 1 - t, me - half + t):

            @pl.when(run >= 0)
            def _():
                load(run).wait()
                hand(run).start()

    load(me).wait()
    hand(me).start()

    def base(run, u):
        s = pl.ds(u * part, part)
        return tiles[core, run, s, :].astype(jnp.float32) + peer[run, s, :].astype(jnp.float32)

    def down_copy(run, u):
        s = pl.ds(u * part, part)
        return send(put_down.at[run, s], got_down.at[run, s], ds.at[run, u], dr.at[run, u], down)

    def up_copy(run, u, put):
        s = pl.ds(u * part, part)
        return send(put.at[run, s], got_up.at[run, s], us.at[run, u], ur.at[run, u], up)

    for t in range(half):
        wrap = me - half - 1 - t
        run = me - half + t

        @pl.when(wrap >= 0)
        def _():
            hand(wrap).wait_recv()
            for u in range(SUB):
                s = pl.ds(u * part, part)
                val = base(wrap, u)
                if t > 0:
                    up_copy(wrap, u, put_up).wait_recv()
                    val = val + got_up[wrap, s, :].astype(jnp.float32)
                put_up[wrap, s, :] = val.astype(jnp.bfloat16)
                up_copy(wrap, u, put_up).start()

        @pl.when(run >= 0)
        def _():
            hand(run).wait_recv()
            for u in range(SUB):
                s = pl.ds(u * part, part)
                if t == 0:
                    put_down[run, s, :] = base(run, u).astype(jnp.bfloat16)
                else:

                    @pl.when(me < last)
                    def _():
                        down_copy(run, u).wait_recv()
                        val = base(run, u) + got_down[run, s, :].astype(jnp.float32)
                        put_down[run, s, :] = val.astype(jnp.bfloat16)

                    @pl.when(me == last)
                    def _():
                        put_down[run, s, :] = base(run, u).astype(jnp.bfloat16)

                down_copy(run, u).start()

    for o in range(wraps - 1, 0, -1):

        @pl.when(me < o)
        def _():
            for u in range(SUB):
                up_copy(o, u, got_up).wait_recv()
                up_copy(o, u, got_up).start()

    hand(me).wait_recv()
    for u in range(SUB):
        s = pl.ds(u * part, part)

        @pl.when(me < last)
        def _():
            down_copy(me, u).wait_recv()

        @pl.when(me < wraps)
        def _():
            up_copy(me, u, got_up).wait_recv()
            final[core, s, :] = (
                base(me, u)
                + got_down[me, s, :].astype(jnp.float32)
                + got_up[me, s, :].astype(jnp.float32)
            ).astype(jnp.bfloat16)

        @pl.when((me >= wraps) & (me < last))
        def _():
            val = base(me, u) + got_down[me, s, :].astype(jnp.float32)
            final[core, s, :] = val.astype(jnp.bfloat16)

        @pl.when(me == last)
        def _():
            final[core, s, :] = base(me, u).astype(jnp.bfloat16)

        send(final.at[core, s], final.at[core, s], fs.at[u], fr.at[u], partner).start()
    for u in range(SUB):
        s = pl.ds(u * part, part)
        send(final.at[core, s], final.at[core, s], fs.at[u], fr.at[u], partner).wait()
    for run in range(n):

        @pl.when(run <= me)
        def _():
            hand(run).wait_send()

        @pl.when((run < me) & (me <= run + half))
        def _():
            for u in range(SUB):
                down_copy(run, u).wait_send()

        if run < wraps:

            @pl.when((me < run) | (me > run + half))
            def _():
                for u in range(SUB):
                    up_copy(run, u, got_up).wait_send()

    out[...] = final[...]


def vmem():
    return pl.BlockSpec(memory_space=pltpu.VMEM)


def anywhere():
    return pl.BlockSpec(memory_space=pl.ANY)


def per_device(queries, grad_out, keys, values, indices, valid):
    tokens, _, heads_here, width = queries.shape
    n = lax.axis_size("seq")
    blocks = tokens // BLK
    total_blocks = n * blocks
    scaling = 1.0 / math.sqrt(width)
    rows = BLK * heads_here
    half = n // 2
    rest = n - 1 - half
    dma = pltpu.SemaphoreType.DMA
    bf16, f32 = jnp.bfloat16, jnp.float32
    picks, usable = indices[0].T, valid[0].T

    kv = pl.pallas_call(
        functools.partial(gather_kernel, n),
        out_shape=jax.ShapeDtypeStruct((2, n, tokens, width), bf16),
        in_specs=[anywhere()] * 2,
        out_specs=vmem(),
        scratch_shapes=[
            dma((2,)),
            dma((n, SUB)), dma((n, SUB)),
            dma((rest, SUB)), dma((rest, SUB)),
            dma((n,)), dma((n,)),
            pltpu.SemaphoreType.REGULAR,
        ],
        compiler_params=pltpu.CompilerParams(collective_id=1, has_side_effects=True),
    )(keys[:, 0], values[:, 0])

    q2 = queries.reshape(tokens * heads_here, width)
    do2 = grad_out.reshape(tokens * heads_here, width)
    full = (2, total_blocks, BLK, width)
    by_block = pl.BlockSpec((rows, width), lambda i, *_: (i, 0))
    dq, tiles = pl.pallas_call(
        functools.partial(attend_kernel, scaling, n),
        out_shape=(
            jax.ShapeDtypeStruct((tokens * heads_here, width), bf16),
            jax.ShapeDtypeStruct(full, bf16),
        ),
        grid_spec=pltpu.PrefetchScalarGridSpec(
            num_scalar_prefetch=2,
            grid=(blocks,),
            in_specs=[by_block, by_block, anywhere()],
            out_specs=[by_block, anywhere()],
            scratch_shapes=[
                pltpu.VMEM(full, f32),
                pltpu.VMEM(full, bf16),
                pltpu.VMEM(full, bf16),
                dma,
                dma((n,)),
            ],
        ),
        compiler_params=pltpu.CompilerParams(
            dimension_semantics=("arbitrary",), vmem_limit_bytes=60 * 2**20
        ),
    )(picks, usable, q2, do2, kv.reshape(full))

    own = pl.pallas_call(
        functools.partial(reduce_kernel, n),
        out_shape=jax.ShapeDtypeStruct((2, tokens, width), bf16),
        in_specs=[anywhere()],
        out_specs=vmem(),
        scratch_shapes=[
            pltpu.VMEM((2, n, tokens, width), bf16),
            dma((n,)),
            pltpu.VMEM((n, tokens, width), bf16),
            pltpu.VMEM((n, tokens, width), bf16),
            pltpu.VMEM((rest, tokens, width), bf16),
            pltpu.VMEM((n, tokens, width), bf16),
            pltpu.VMEM((rest, tokens, width), bf16),
            pltpu.VMEM((2, tokens, width), bf16),
            dma((n, SUB)), dma((n, SUB)),
            dma((rest, SUB)), dma((rest, SUB)),
            dma((n,)), dma((n,)),
            dma((SUB,)), dma((SUB,)),
        ],
        compiler_params=pltpu.CompilerParams(
            collective_id=2, has_side_effects=True, vmem_limit_bytes=60 * 2**20
        ),
    )(tiles.reshape(2, n, tokens, width))
    gk, gv = own[0], own[1]
    return (
        dq.reshape(tokens, 1, heads_here, width),
        gk.reshape(tokens, 1, width),
        gv.reshape(tokens, 1, width),
    )


def solution(mesh):
    return jax.shard_map(
        per_device,
        mesh=mesh,
        in_specs=(
            P(("groups", "seq"), "head", "inner", None),
            P(("groups", "seq"), "head", "inner", None),
            P(("groups", "seq"), "head", None),
            P(("groups", "seq"), "head", None),
            P("head", "groups", None),
            P("head", "groups", None),
        ),
        out_specs=(
            P(("groups", "seq"), "head", "inner", None),
            P(("groups", "seq"), "head", None),
            P(("groups", "seq"), "head", None),
        ),
        check_vma=False,
    )
```

```python
import functools
import math

import jax
import jax.numpy as jnp
from jax import lax
from jax.experimental import pallas as pl
from jax.experimental.pallas import tpu as pltpu
from jax.sharding import PartitionSpec as P

BLK = 64
TOPK = 16
SUB = 4
MESH = pl.DeviceIdType.MESH
LOG2E = 1.4426950408889634


def greet(n):
    me = lax.axis_index("seq")
    core = lax.axis_index("inner")
    barrier = pltpu.get_barrier_semaphore()
    peers = ({"seq": lax.rem(me + 1, n)}, {"seq": lax.rem(me + n - 1, n)}, {"inner": 1 - core})
    for where in peers:
        pl.semaphore_signal(barrier, inc=1, device_id=where, device_id_type=MESH)
    pl.semaphore_wait(barrier, len(peers))


def send(src, dst, s_sem, r_sem, where):
    return pltpu.make_async_remote_copy(
        src_ref=src, dst_ref=dst, send_sem=s_sem, recv_sem=r_sem, device_id=where, device_id_type=MESH
    )


def gather_kernel(n, sub, k_ref, v_ref, kv_ref, local_sem, ss, rs, ps, pr):
    me = lax.axis_index("seq")
    core = lax.axis_index("inner")
    way = 1 - 2 * core
    ahead = {"seq": lax.rem(me + way + n, n)}
    partner = {"inner": 1 - core}
    part = k_ref.shape[0] // sub
    half = n // 2
    own_k = pltpu.make_async_copy(k_ref, kv_ref.at[0, me], local_sem.at[0])
    own_v = pltpu.make_async_copy(v_ref, kv_ref.at[1, me], local_sem.at[1])
    own_k.start()
    own_v.start()
    greet(n)
    own_k.wait()
    own_v.wait()

    def run_of(t):
        return lax.rem(me - way * t + n, n)

    def pieces(t):
        if t == half - 1:
            return [(core, u, u) for u in range(sub)]
        return [(a, u, a * sub + u) for u in range(sub) for a in range(2)]

    def hop(t, a, u, j):
        ref = kv_ref.at[a, run_of(t), pl.ds(u * part, part)]
        return send(ref, ref, ss.at[t, j], rs.at[t, j], ahead)

    def share(t):
        if t == half:
            ref = kv_ref.at[core, run_of(t)]
        else:
            ref = kv_ref.at[:, run_of(t)]
        return send(ref, ref, ps.at[t], pr.at[t], partner)

    def landed(t):
        run = lax.rem(me + way * t + n, n)
        if t == half:
            ref = kv_ref.at[1 - core, run]
        else:
            ref = kv_ref.at[:, run]
        return send(ref, ref, ps.at[t], pr.at[t], partner)

    for p in pieces(0):
        hop(0, *p).start()
    for t in range(half):
        later = pieces(t + 1) if t + 1 < half else []
        for a, u, j in pieces(t):
            ref = kv_ref.at[a, run_of(t + 1), pl.ds(u * part, part)]
            send(ref, ref, ss.at[t, j], rs.at[t, j], ahead).wait_recv()
            if t + 1 < half - 1:
                hop(t + 1, a, u, j).start()
        if t + 1 == half - 1:
            for p in later:
                hop(t + 1, *p).start()
        share(t + 1).start()
    for t in range(1, half + 1):
        landed(t).wait_recv()
        share(t).wait_send()
    for t in range(half):
        for p in pieces(t):
            hop(t, *p).wait_send()


def attend_kernel(scaling, picks, usable, q_ref, do_ref, kv_ref, dq_ref, tiles_ref, acc):
    i = pl.program_id(0)
    at = lax.axis_index("seq") * pl.num_programs(0) + i
    rows = q_ref.shape[0]
    per_pos = rows // BLK

    @pl.when(i == 0)
    def _():
        acc[...] = jnp.zeros_like(acc)

    q = q_ref[...]
    do = do_ref[...]
    names = [jnp.where(usable[t, at] > 0, picks[t, at], at) for t in range(TOPK)]
    ks = jnp.concatenate([kv_ref[0, b] for b in names], axis=0)
    vs = jnp.concatenate([kv_ref[1, b] for b in names], axis=0)
    nt = (((1,), (1,)), ((), ()))
    st = lax.dot_general(ks, q, nt, preferred_element_type=jnp.float32)
    key_at = lax.broadcasted_iota(jnp.int32, (BLK, rows), 0)
    query_at = lax.broadcasted_iota(jnp.int32, (BLK, rows), 1) // per_pos
    low = jnp.float32(-1e30)
    parts = [jnp.where(key_at <= query_at, st[:BLK], low)]
    for t in range(1, TOPK):
        bias = jnp.where(usable[t, at] > 0, jnp.float32(0.0), low)
        parts.append(st[t * BLK : (t + 1) * BLK] + bias)
    st = jnp.concatenate(parts, axis=0)
    top = jnp.max(st, axis=0, keepdims=True)
    w = jnp.exp2((st - top) * jnp.float32(scaling * LOG2E))
    inv = 1.0 / jnp.sum(w, axis=0, keepdims=True)
    p = w * inv
    dp = lax.dot_general(vs, do, nt, preferred_element_type=jnp.float32)
    delta = jnp.sum(p * dp, axis=0, keepdims=True)
    dsc = (p * (dp - delta)).astype(jnp.bfloat16)
    pb = p.astype(jnp.bfloat16)
    dqt = lax.dot_general(ks, dsc, (((0,), (0,)), ((), ())), preferred_element_type=jnp.float32)
    dq_ref[...] = (dqt.T * scaling).astype(jnp.bfloat16)
    dk = jnp.dot(dsc, q, preferred_element_type=jnp.float32) * scaling
    dv = jnp.dot(pb, do, preferred_element_type=jnp.float32)
    for t in range(TOPK):
        acc[0, names[t]] += dk[t * BLK : (t + 1) * BLK]
        acc[1, names[t]] += dv[t * BLK : (t + 1) * BLK]

    @pl.when(i == pl.num_programs(0) - 1)
    def _():
        tiles_ref[...] = acc[...].astype(jnp.bfloat16)


def reduce_kernel(n, sub, tiles, out, peer, put, got, mine, theirs, ss, rs, ps, pr, fs, fr):
    me = lax.axis_index("seq")
    core = lax.axis_index("inner")
    way = 1 - 2 * core
    ahead = {"seq": lax.rem(me - way + n, n)}
    partner = {"inner": 1 - core}
    part = tiles.shape[2] // sub
    half = n // 2
    f32, bf16 = jnp.float32, jnp.bfloat16
    greet(n)

    def owner(t, way):
        return lax.rem(me - way * (half - t) + 2 * n, n)

    def hand(t):
        run = owner(t, -way)
        if t == 0:
            src, dst = tiles.at[1 - core, run], peer.at[1 - core, t]
        else:
            src, dst = tiles.at[:, run], peer.at[:, t]
        return send(src, dst, ps.at[t], pr.at[t], partner)

    def landed(t):
        if t == 0:
            ref = peer.at[core, t]
        else:
            ref = peer.at[:, t]
        return send(ref, ref, ps.at[t], pr.at[t], partner)

    def pieces(t):
        if t == 0:
            return [(core, u, u) for u in range(sub)]
        return [(a, u, a * sub + u) for u in range(sub) for a in range(2)]

    def hop(t, a, u, j):
        s = pl.ds(u * part, part)
        return send(put.at[a, t, s], got.at[a, t, s], ss.at[t, j], rs.at[t, j], ahead)

    for t in range(half):
        hand(t).start()
    for t in range(half):
        landed(t).wait_recv()
        run = owner(t, way)
        if t == 1:
            for p in pieces(0):
                hop(0, *p).wait_recv()
        for a, u, j in pieces(t):
            s = pl.ds(u * part, part)
            val = tiles[a, run, s, :].astype(f32) + peer[a, t, s, :].astype(f32)
            if t == 1:
                come = got[a, 0, s, :].astype(f32)
                val = val + jnp.where(core == a, come, 0.0)
            elif t > 1:
                hop(t - 1, a, u, j).wait_recv()
                val = val + got[a, t - 1, s, :].astype(f32)
            put[a, t, s, :] = val.astype(bf16)
            hop(t, a, u, j).start()
    swaps = []
    for a, u, j in pieces(half - 1):
        s = pl.ds(u * part, part)
        hop(half - 1, a, u, j).wait_recv()
        mine[a, s, :] = (tiles[a, me, s, :].astype(f32) + got[a, half - 1, s, :].astype(f32)).astype(bf16)
        c = send(mine.at[a, s], theirs.at[a, s], fs.at[j], fr.at[j], partner)
        c.start()
        swaps.append((c, a, s))
    for c, a, s in swaps:
        c.wait_recv()
        out[a, s, :] = (mine[a, s, :].astype(f32) + theirs[a, s, :].astype(f32)).astype(bf16)
    for c, a, s in swaps:
        c.wait_send()
    for t in range(half):
        hand(t).wait_send()
        for p in pieces(t):
            hop(t, *p).wait_send()


def vmem():
    return pl.BlockSpec(memory_space=pltpu.VMEM)


def anywhere():
    return pl.BlockSpec(memory_space=pl.ANY)


def per_device(queries, grad_out, keys, values, indices, valid):
    tokens, _, heads_here, width = queries.shape
    n = lax.axis_size("seq")
    blocks = tokens // BLK
    total_blocks = n * blocks
    scaling = 1.0 / math.sqrt(width)
    rows = BLK * heads_here
    half = n // 2
    dma = pltpu.SemaphoreType.DMA
    bf16, f32 = jnp.bfloat16, jnp.float32
    picks, usable = indices[0].T, valid[0].T

    kv = pl.pallas_call(
        functools.partial(gather_kernel, n, SUB),
        out_shape=jax.ShapeDtypeStruct((2, n, tokens, width), bf16),
        in_specs=[anywhere()] * 2,
        out_specs=vmem(),
        scratch_shapes=[
            dma((2,)),
            dma((half, 2 * SUB)), dma((half, 2 * SUB)),
            dma((half + 1,)), dma((half + 1,)),
        ],
        compiler_params=pltpu.CompilerParams(collective_id=1, has_side_effects=True),
    )(keys[:, 0], values[:, 0])

    q2 = queries.reshape(tokens * heads_here, width)
    do2 = grad_out.reshape(tokens * heads_here, width)
    full = (2, total_blocks, BLK, width)
    whole = lambda i, *_: (0, 0, 0, 0)
    by_block = pl.BlockSpec((rows, width), lambda i, *_: (i, 0))
    dq, tiles = pl.pallas_call(
        functools.partial(attend_kernel, scaling),
        out_shape=(
            jax.ShapeDtypeStruct((tokens * heads_here, width), bf16),
            jax.ShapeDtypeStruct(full, bf16),
        ),
        grid_spec=pltpu.PrefetchScalarGridSpec(
            num_scalar_prefetch=2,
            grid=(blocks,),
            in_specs=[by_block, by_block, pl.BlockSpec(full, whole)],
            out_specs=[by_block, pl.BlockSpec(full, whole)],
            scratch_shapes=[pltpu.VMEM(full, f32)],
        ),
        compiler_params=pltpu.CompilerParams(
            dimension_semantics=("arbitrary",), vmem_limit_bytes=60 * 2**20
        ),
    )(picks, usable, q2, do2, kv.reshape(full))

    own = pl.pallas_call(
        functools.partial(reduce_kernel, n, SUB),
        out_shape=jax.ShapeDtypeStruct((2, tokens, width), bf16),
        in_specs=[vmem()],
        out_specs=vmem(),
        scratch_shapes=[
            pltpu.VMEM((2, half, tokens, width), bf16),
            pltpu.VMEM((2, half, tokens, width), bf16),
            pltpu.VMEM((2, half, tokens, width), bf16),
            pltpu.VMEM((2, tokens, width), bf16),
            pltpu.VMEM((2, tokens, width), bf16),
            dma((half, 2 * SUB)), dma((half, 2 * SUB)),
            dma((half,)), dma((half,)),
            dma((2 * SUB,)), dma((2 * SUB,)),
        ],
        compiler_params=pltpu.CompilerParams(
            collective_id=2, has_side_effects=True, vmem_limit_bytes=60 * 2**20
        ),
    )(tiles.reshape(2, n, tokens, width))
    gk, gv = own[0], own[1]
    return (
        dq.reshape(tokens, 1, heads_here, width),
        gk.reshape(tokens, 1, width),
        gv.reshape(tokens, 1, width),
    )


def solution(mesh):
    return jax.shard_map(
        per_device,
        mesh=mesh,
        in_specs=(
            P(("groups", "seq"), "head", "inner", None),
            P(("groups", "seq"), "head", "inner", None),
            P(("groups", "seq"), "head", None),
            P(("groups", "seq"), "head", None),
            P("head", "groups", None),
            P("head", "groups", None),
        ),
        out_specs=(
            P(("groups", "seq"), "head", "inner", None),
            P(("groups", "seq"), "head", None),
            P(("groups", "seq"), "head", None),
        ),
        check_vma=False,
    )
```

```python
import functools
import math

import jax
import jax.numpy as jnp
from jax import lax
from jax.experimental import pallas as pl
from jax.experimental.pallas import tpu as pltpu
from jax.sharding import PartitionSpec as P

BLK = 64
TOPK = 16
SUB = 4
MESH = pl.DeviceIdType.MESH
LOG2E = 1.4426950408889634


def greet(n):
    me = lax.axis_index("seq")
    core = lax.axis_index("inner")
    barrier = pltpu.get_barrier_semaphore()
    peers = ({"seq": lax.rem(me + 1, n)}, {"seq": lax.rem(me + n - 1, n)}, {"inner": 1 - core})
    for where in peers:
        pl.semaphore_signal(barrier, inc=1, device_id=where, device_id_type=MESH)
    pl.semaphore_wait(barrier, len(peers))


def send(src, dst, s_sem, r_sem, where):
    return pltpu.make_async_remote_copy(
        src_ref=src, dst_ref=dst, send_sem=s_sem, recv_sem=r_sem, device_id=where, device_id_type=MESH
    )


def gather_kernel(n, sub, k_ref, v_ref, kv_ref, local_sem, ss, rs, ps, pr):
    me = lax.axis_index("seq")
    core = lax.axis_index("inner")
    way = 1 - 2 * core
    ahead = {"seq": lax.rem(me + way + n, n)}
    partner = {"inner": 1 - core}
    part = k_ref.shape[0] // sub
    half = n // 2
    own_k = pltpu.make_async_copy(k_ref, kv_ref.at[0, me], local_sem.at[0])
    own_v = pltpu.make_async_copy(v_ref, kv_ref.at[1, me], local_sem.at[1])
    own_k.start()
    own_v.start()
    greet(n)
    own_k.wait()
    own_v.wait()

    def run_of(t):
        return lax.rem(me - way * t + n, n)

    def pieces(t):
        if t == half - 1:
            return [(core, u, u) for u in range(sub)]
        return [(a, u, a * sub + u) for u in range(sub) for a in range(2)]

    def hop(t, a, u, j):
        ref = kv_ref.at[a, run_of(t), pl.ds(u * part, part)]
        return send(ref, ref, ss.at[t, j], rs.at[t, j], ahead)

    def share(t):
        if t == half:
            ref = kv_ref.at[core, run_of(t)]
        else:
            ref = kv_ref.at[:, run_of(t)]
        return send(ref, ref, ps.at[t], pr.at[t], partner)

    def landed(t):
        run = lax.rem(me + way * t + n, n)
        if t == half:
            ref = kv_ref.at[1 - core, run]
        else:
            ref = kv_ref.at[:, run]
        return send(ref, ref, ps.at[t], pr.at[t], partner)

    for p in pieces(0):
        hop(0, *p).start()
    for t in range(half):
        later = pieces(t + 1) if t + 1 < half else []
        for a, u, j in pieces(t):
            ref = kv_ref.at[a, run_of(t + 1), pl.ds(u * part, part)]
            send(ref, ref, ss.at[t, j], rs.at[t, j], ahead).wait_recv()
            if t + 1 < half - 1:
                hop(t + 1, a, u, j).start()
        if t + 1 == half - 1:
            for p in later:
                hop(t + 1, *p).start()
        share(t + 1).start()
    for t in range(1, half + 1):
        landed(t).wait_recv()
        share(t).wait_send()
    for t in range(half):
        for p in pieces(t):
            hop(t, *p).wait_send()


def attend_kernel(scaling, picks, usable, q_ref, do_ref, kv_ref, dq_ref, tiles_ref, acc):
    i = pl.program_id(0)
    at = lax.axis_index("seq") * pl.num_programs(0) + i
    rows = q_ref.shape[0]
    per_pos = rows // BLK

    @pl.when(i == 0)
    def _():
        acc[...] = jnp.zeros_like(acc)

    q = q_ref[...]
    do = do_ref[...]
    names = [jnp.where(usable[t, at] > 0, picks[t, at], at) for t in range(TOPK)]
    ks = jnp.concatenate([kv_ref[0, b] for b in names], axis=0)
    vs = jnp.concatenate([kv_ref[1, b] for b in names], axis=0)
    nt = (((1,), (1,)), ((), ()))
    st = lax.dot_general(ks, q, nt, preferred_element_type=jnp.float32)
    key_at = lax.broadcasted_iota(jnp.int32, (BLK, rows), 0)
    query_at = lax.broadcasted_iota(jnp.int32, (BLK, rows), 1) // per_pos
    low = jnp.float32(-1e30)
    parts = [jnp.where(key_at <= query_at, st[:BLK], low)]
    for t in range(1, TOPK):
        bias = jnp.where(usable[t, at] > 0, jnp.float32(0.0), low)
        parts.append(st[t * BLK : (t + 1) * BLK] + bias)
    st = jnp.concatenate(parts, axis=0)
    top = jnp.max(st, axis=0, keepdims=True)
    w = jnp.exp2((st - top) * jnp.float32(scaling * LOG2E))
    inv = 1.0 / jnp.sum(w, axis=0, keepdims=True)
    p = w * inv
    dp = lax.dot_general(vs, do, nt, preferred_element_type=jnp.float32)
    delta = jnp.sum(p * dp, axis=0, keepdims=True)
    dsc = (p * (dp - delta)).astype(jnp.bfloat16)
    pb = p.astype(jnp.bfloat16)
    dqt = lax.dot_general(ks, dsc, (((0,), (0,)), ((), ())), preferred_element_type=jnp.float32)
    dq_ref[...] = (dqt.T * scaling).astype(jnp.bfloat16)
    dk = jnp.dot(dsc, q, preferred_element_type=jnp.float32) * scaling
    dv = jnp.dot(pb, do, preferred_element_type=jnp.float32)
    for t in range(TOPK):
        acc[0, names[t]] += dk[t * BLK : (t + 1) * BLK]
        acc[1, names[t]] += dv[t * BLK : (t + 1) * BLK]

    @pl.when(i == pl.num_programs(0) - 1)
    def _():
        tiles_ref[...] = acc[...].astype(jnp.bfloat16)


def reduce_kernel(n, sub, tiles, out, peer, put, got, mine, theirs, ss, rs, ps, pr, fs, fr):
    me = lax.axis_index("seq")
    core = lax.axis_index("inner")
    way = 1 - 2 * core
    ahead = {"seq": lax.rem(me - way + n, n)}
    partner = {"inner": 1 - core}
    part = tiles.shape[2] // sub
    half = n // 2
    f32, bf16 = jnp.float32, jnp.bfloat16
    greet(n)

    def owner(t, way):
        return lax.rem(me - way * (half - t) + 2 * n, n)

    def hand(t):
        run = owner(t, -way)
        if t == 0:
            src, dst = tiles.at[1 - core, run], peer.at[1 - core, t]
        else:
            src, dst = tiles.at[:, run], peer.at[:, t]
        return send(src, dst, ps.at[t], pr.at[t], partner)

    def landed(t):
        if t == 0:
            ref = peer.at[core, t]
        else:
            ref = peer.at[:, t]
        return send(ref, ref, ps.at[t], pr.at[t], partner)

    def pieces(t):
        if t == 0:
            return [(core, u, u) for u in range(sub)]
        return [(a, u, a * sub + u) for u in range(sub) for a in range(2)]

    def hop(t, a, u, j):
        s = pl.ds(u * part, part)
        return send(put.at[a, t, s], got.at[a, t, s], ss.at[t, j], rs.at[t, j], ahead)

    for t in range(half):
        hand(t).start()
    for t in range(half):
        landed(t).wait_recv()
        run = owner(t, way)
        if t == 1:
            for p in pieces(0):
                hop(0, *p).wait_recv()
        for a, u, j in pieces(t):
            s = pl.ds(u * part, part)
            val = tiles[a, run, s, :].astype(f32) + peer[a, t, s, :].astype(f32)
            if t == 1:
                come = got[a, 0, s, :].astype(f32)
                val = val + jnp.where(core == a, come, 0.0)
            elif t > 1:
                hop(t - 1, a, u, j).wait_recv()
                val = val + got[a, t - 1, s, :].astype(f32)
            put[a, t, s, :] = val.astype(bf16)
            hop(t, a, u, j).start()
    swaps = []
    for a, u, j in pieces(half - 1):
        s = pl.ds(u * part, part)
        hop(half - 1, a, u, j).wait_recv()
        mine[a, s, :] = (tiles[a, me, s, :].astype(f32) + got[a, half - 1, s, :].astype(f32)).astype(bf16)
        c = send(mine.at[a, s], theirs.at[a, s], fs.at[j], fr.at[j], partner)
        c.start()
        swaps.append((c, a, s))
    for c, a, s in swaps:
        c.wait_recv()
        out[a, s, :] = (mine[a, s, :].astype(f32) + theirs[a, s, :].astype(f32)).astype(bf16)
    for c, a, s in swaps:
        c.wait_send()
    for t in range(half):
        hand(t).wait_send()
        for p in pieces(t):
            hop(t, *p).wait_send()


def vmem():
    return pl.BlockSpec(memory_space=pltpu.VMEM)


def anywhere():
    return pl.BlockSpec(memory_space=pl.ANY)


def per_device(queries, grad_out, keys, values, indices, valid):
    tokens, _, heads_here, width = queries.shape
    n = lax.axis_size("seq")
    blocks = tokens // BLK
    total_blocks = n * blocks
    scaling = 1.0 / math.sqrt(width)
    rows = BLK * heads_here
    half = n // 2
    dma = pltpu.SemaphoreType.DMA
    bf16, f32 = jnp.bfloat16, jnp.float32
    picks, usable = indices[0].T, valid[0].T

    kv = pl.pallas_call(
        functools.partial(gather_kernel, n, SUB),
        out_shape=jax.ShapeDtypeStruct((2, n, tokens, width), bf16),
        in_specs=[anywhere()] * 2,
        out_specs=vmem(),
        scratch_shapes=[
            dma((2,)),
            dma((half, 2 * SUB)), dma((half, 2 * SUB)),
            dma((half + 1,)), dma((half + 1,)),
        ],
        compiler_params=pltpu.CompilerParams(collective_id=1, has_side_effects=True, vmem_limit_bytes=12 * 2**20),
    )(keys[:, 0], values[:, 0])

    q2 = queries.reshape(tokens * heads_here, width)
    do2 = grad_out.reshape(tokens * heads_here, width)
    full = (2, total_blocks, BLK, width)
    whole = lambda i, *_: (0, 0, 0, 0)
    by_block = pl.BlockSpec((rows, width), lambda i, *_: (i, 0))
    dq, tiles = pl.pallas_call(
        functools.partial(attend_kernel, scaling),
        out_shape=(
            jax.ShapeDtypeStruct((tokens * heads_here, width), bf16),
            jax.ShapeDtypeStruct(full, bf16),
        ),
        grid_spec=pltpu.PrefetchScalarGridSpec(
            num_scalar_prefetch=2,
            grid=(blocks,),
            in_specs=[by_block, by_block, pl.BlockSpec(full, whole)],
            out_specs=[by_block, pl.BlockSpec(full, whole)],
            scratch_shapes=[pltpu.VMEM(full, f32)],
        ),
        compiler_params=pltpu.CompilerParams(
            dimension_semantics=("arbitrary",), vmem_limit_bytes=34 * 2**20
        ),
    )(picks, usable, q2, do2, kv.reshape(full))

    own = pl.pallas_call(
        functools.partial(reduce_kernel, n, SUB),
        out_shape=jax.ShapeDtypeStruct((2, tokens, width), bf16),
        in_specs=[vmem()],
        out_specs=vmem(),
        scratch_shapes=[
            pltpu.VMEM((2, half, tokens, width), bf16),
            pltpu.VMEM((2, half, tokens, width), bf16),
            pltpu.VMEM((2, half, tokens, width), bf16),
            pltpu.VMEM((2, tokens, width), bf16),
            pltpu.VMEM((2, tokens, width), bf16),
            dma((half, 2 * SUB)), dma((half, 2 * SUB)),
            dma((half,)), dma((half,)),
            dma((2 * SUB,)), dma((2 * SUB,)),
        ],
        compiler_params=pltpu.CompilerParams(
            collective_id=2, has_side_effects=True, vmem_limit_bytes=28 * 2**20
        ),
    )(tiles.reshape(2, n, tokens, width))
    gk, gv = own[0], own[1]
    return (
        dq.reshape(tokens, 1, heads_here, width),
        gk.reshape(tokens, 1, width),
        gv.reshape(tokens, 1, width),
    )


def solution(mesh):
    return jax.shard_map(
        per_device,
        mesh=mesh,
        in_specs=(
            P(("groups", "seq"), "head", "inner", None),
            P(("groups", "seq"), "head", "inner", None),
            P(("groups", "seq"), "head", None),
            P(("groups", "seq"), "head", None),
            P("head", "groups", None),
            P("head", "groups", None),
        ),
        out_specs=(
            P(("groups", "seq"), "head", "inner", None),
            P(("groups", "seq"), "head", None),
            P(("groups", "seq"), "head", None),
        ),
        check_vma=False,
    )
```

```python
import functools
import math

import jax
import jax.numpy as jnp
from jax import lax
from jax.experimental import pallas as pl
from jax.experimental.pallas import tpu as pltpu
from jax.sharding import PartitionSpec as P

BLK = 64
TOPK = 16
SUB = 4
TOGETHER = 2
MESH = pl.DeviceIdType.MESH
LOG2E = 1.4426950408889634


def greet(n):
    me = lax.axis_index("seq")
    core = lax.axis_index("inner")
    barrier = pltpu.get_barrier_semaphore()
    peers = ({"seq": lax.rem(me + 1, n)}, {"seq": lax.rem(me + n - 1, n)}, {"inner": 1 - core})
    for where in peers:
        pl.semaphore_signal(barrier, inc=1, device_id=where, device_id_type=MESH)
    pl.semaphore_wait(barrier, len(peers))


def send(src, dst, s_sem, r_sem, where):
    return pltpu.make_async_remote_copy(
        src_ref=src, dst_ref=dst, send_sem=s_sem, recv_sem=r_sem, device_id=where, device_id_type=MESH
    )


def gather_kernel(n, sub, k_ref, v_ref, kv_ref, local_sem, ss, rs, ps, pr):
    me = lax.axis_index("seq")
    core = lax.axis_index("inner")
    way = 1 - 2 * core
    ahead = {"seq": lax.rem(me + way + n, n)}
    partner = {"inner": 1 - core}
    part = k_ref.shape[0] // sub
    half = n // 2
    own_k = pltpu.make_async_copy(k_ref, kv_ref.at[0, me], local_sem.at[0])
    own_v = pltpu.make_async_copy(v_ref, kv_ref.at[1, me], local_sem.at[1])
    own_k.start()
    own_v.start()
    greet(n)
    own_k.wait()
    own_v.wait()

    def run_of(t):
        return lax.rem(me - way * t + n, n)

    def pieces(t):
        if t == half - 1:
            return [(core, u, u) for u in range(sub)]
        return [(a, u, a * sub + u) for u in range(sub) for a in range(2)]

    def hop(t, a, u, j):
        ref = kv_ref.at[a, run_of(t), pl.ds(u * part, part)]
        return send(ref, ref, ss.at[t, j], rs.at[t, j], ahead)

    def share(t):
        if t == half:
            ref = kv_ref.at[core, run_of(t)]
        else:
            ref = kv_ref.at[:, run_of(t)]
        return send(ref, ref, ps.at[t], pr.at[t], partner)

    def landed(t):
        run = lax.rem(me + way * t + n, n)
        if t == half:
            ref = kv_ref.at[1 - core, run]
        else:
            ref = kv_ref.at[:, run]
        return send(ref, ref, ps.at[t], pr.at[t], partner)

    for p in pieces(0):
        hop(0, *p).start()
    for t in range(half):
        later = pieces(t + 1) if t + 1 < half else []
        for a, u, j in pieces(t):
            ref = kv_ref.at[a, run_of(t + 1), pl.ds(u * part, part)]
            send(ref, ref, ss.at[t, j], rs.at[t, j], ahead).wait_recv()
            if t + 1 < half - 1:
                hop(t + 1, a, u, j).start()
        if t + 1 == half - 1:
            for p in later:
                hop(t + 1, *p).start()
        share(t + 1).start()
    for t in range(1, half + 1):
        landed(t).wait_recv()
        share(t).wait_send()
    for t in range(half):
        for p in pieces(t):
            hop(t, *p).wait_send()


def attend_block(scaling, at, picks, usable, q, do, kv_ref):
    rows = q.shape[0]
    per_pos = rows // BLK
    names = [jnp.where(usable[t, at] > 0, picks[t, at], at) for t in range(TOPK)]
    ks = jnp.concatenate([kv_ref[0, b] for b in names], axis=0)
    vs = jnp.concatenate([kv_ref[1, b] for b in names], axis=0)
    nt = (((1,), (1,)), ((), ()))
    st = lax.dot_general(ks, q, nt, preferred_element_type=jnp.float32)
    dp = lax.dot_general(vs, do, nt, preferred_element_type=jnp.float32)
    key_at = lax.broadcasted_iota(jnp.int32, (BLK, rows), 0)
    query_at = lax.broadcasted_iota(jnp.int32, (BLK, rows), 1) // per_pos
    low = jnp.float32(-1e30)
    parts = [jnp.where(key_at <= query_at, st[:BLK], low)]
    for t in range(1, TOPK):
        bias = jnp.where(usable[t, at] > 0, jnp.float32(0.0), low)
        parts.append(st[t * BLK : (t + 1) * BLK] + bias)
    st = jnp.concatenate(parts, axis=0)
    top = jnp.max(st, axis=0, keepdims=True)
    w = jnp.exp2((st - top) * jnp.float32(scaling * LOG2E))
    inv = 1.0 / jnp.sum(w, axis=0, keepdims=True)
    p = w * inv
    delta = jnp.sum(p * dp, axis=0, keepdims=True)
    dsc = (p * (dp - delta)).astype(jnp.bfloat16)
    pb = p.astype(jnp.bfloat16)
    dqt = lax.dot_general(ks, dsc, (((0,), (0,)), ((), ())), preferred_element_type=jnp.float32)
    dq = (dqt.T * scaling).astype(jnp.bfloat16)
    dk = jnp.dot(dsc, q, preferred_element_type=jnp.float32) * scaling
    dv = jnp.dot(pb, do, preferred_element_type=jnp.float32)
    return names, dq, dk, dv


def attend_kernel(scaling, rows, picks, usable, q_ref, do_ref, kv_ref, dq_ref, tiles_ref, acc):
    i = pl.program_id(0)
    steps = pl.num_programs(0)
    here = q_ref.shape[0] // rows
    at = (lax.axis_index("seq") * steps + i) * here

    @pl.when(i == 0)
    def _():
        acc[...] = jnp.zeros_like(acc)

    done = []
    for b in range(here):
        s = slice(b * rows, (b + 1) * rows)
        done.append(attend_block(scaling, at + b, picks, usable, q_ref[s], do_ref[s], kv_ref))
    for b in range(here):
        names, dq, dk, dv = done[b]
        dq_ref[b * rows : (b + 1) * rows] = dq
        for t in range(TOPK):
            acc[0, names[t]] += dk[t * BLK : (t + 1) * BLK]
            acc[1, names[t]] += dv[t * BLK : (t + 1) * BLK]

    @pl.when(i == steps - 1)
    def _():
        tiles_ref[...] = acc[...].astype(jnp.bfloat16)


def reduce_kernel(n, sub, tiles, out, peer, put, got, mine, theirs, ss, rs, ps, pr, fs, fr):
    me = lax.axis_index("seq")
    core = lax.axis_index("inner")
    way = 1 - 2 * core
    ahead = {"seq": lax.rem(me - way + n, n)}
    partner = {"inner": 1 - core}
    part = tiles.shape[2] // sub
    half = n // 2
    f32, bf16 = jnp.float32, jnp.bfloat16
    greet(n)

    def owner(t, way):
        return lax.rem(me - way * (half - t) + 2 * n, n)

    def hand(t):
        run = owner(t, -way)
        if t == 0:
            src, dst = tiles.at[1 - core, run], peer.at[1 - core, t]
        else:
            src, dst = tiles.at[:, run], peer.at[:, t]
        return send(src, dst, ps.at[t], pr.at[t], partner)

    def landed(t):
        if t == 0:
            ref = peer.at[core, t]
        else:
            ref = peer.at[:, t]
        return send(ref, ref, ps.at[t], pr.at[t], partner)

    def pieces(t):
        if t == 0:
            return [(core, u, u) for u in range(sub)]
        return [(a, u, a * sub + u) for u in range(sub) for a in range(2)]

    def hop(t, a, u, j):
        s = pl.ds(u * part, part)
        return send(put.at[a, t, s], got.at[a, t, s], ss.at[t, j], rs.at[t, j], ahead)

    for t in range(half):
        hand(t).start()
    for t in range(half):
        landed(t).wait_recv()
        run = owner(t, way)
        if t == 1:
            for p in pieces(0):
                hop(0, *p).wait_recv()
        for a, u, j in pieces(t):
            s = pl.ds(u * part, part)
            val = tiles[a, run, s, :].astype(f32) + peer[a, t, s, :].astype(f32)
            if t == 1:
                come = got[a, 0, s, :].astype(f32)
                val = val + jnp.where(core == a, come, 0.0)
            elif t > 1:
                hop(t - 1, a, u, j).wait_recv()
                val = val + got[a, t - 1, s, :].astype(f32)
            put[a, t, s, :] = val.astype(bf16)
            hop(t, a, u, j).start()
    swaps = []
    for a, u, j in pieces(half - 1):
        s = pl.ds(u * part, part)
        hop(half - 1, a, u, j).wait_recv()
        mine[a, s, :] = (tiles[a, me, s, :].astype(f32) + got[a, half - 1, s, :].astype(f32)).astype(bf16)
        c = send(mine.at[a, s], theirs.at[a, s], fs.at[j], fr.at[j], partner)
        c.start()
        swaps.append((c, a, s))
    for c, a, s in swaps:
        c.wait_recv()
        out[a, s, :] = (mine[a, s, :].astype(f32) + theirs[a, s, :].astype(f32)).astype(bf16)
    for c, a, s in swaps:
        c.wait_send()
    for t in range(half):
        hand(t).wait_send()
        for p in pieces(t):
            hop(t, *p).wait_send()


def vmem():
    return pl.BlockSpec(memory_space=pltpu.VMEM)


def anywhere():
    return pl.BlockSpec(memory_space=pl.ANY)


def per_device(queries, grad_out, keys, values, indices, valid):
    tokens, _, heads_here, width = queries.shape
    n = lax.axis_size("seq")
    blocks = tokens // BLK
    total_blocks = n * blocks
    scaling = 1.0 / math.sqrt(width)
    rows = BLK * heads_here
    half = n // 2
    dma = pltpu.SemaphoreType.DMA
    bf16, f32 = jnp.bfloat16, jnp.float32
    picks, usable = indices[0].T, valid[0].T

    kv = pl.pallas_call(
        functools.partial(gather_kernel, n, SUB),
        out_shape=jax.ShapeDtypeStruct((2, n, tokens, width), bf16),
        in_specs=[pl.BlockSpec(memory_space=pltpu.HBM)] * 2,
        out_specs=vmem(),
        scratch_shapes=[
            dma((2,)),
            dma((half, 2 * SUB)), dma((half, 2 * SUB)),
            dma((half + 1,)), dma((half + 1,)),
        ],
        compiler_params=pltpu.CompilerParams(collective_id=1, has_side_effects=True, vmem_limit_bytes=12 * 2**20),
    )(keys[:, 0], values[:, 0])

    q2 = queries.reshape(tokens * heads_here, width)
    do2 = grad_out.reshape(tokens * heads_here, width)
    full = (2, total_blocks, BLK, width)
    whole = lambda i, *_: (0, 0, 0, 0)
    by_block = pl.BlockSpec((TOGETHER * rows, width), lambda i, *_: (i, 0))
    dq, tiles = pl.pallas_call(
        functools.partial(attend_kernel, scaling, rows),
        out_shape=(
            jax.ShapeDtypeStruct((tokens * heads_here, width), bf16),
            jax.ShapeDtypeStruct(full, bf16),
        ),
        grid_spec=pltpu.PrefetchScalarGridSpec(
            num_scalar_prefetch=2,
            grid=(blocks // TOGETHER,),
            in_specs=[by_block, by_block, pl.BlockSpec(full, whole)],
            out_specs=[by_block, pl.BlockSpec(full, whole)],
            scratch_shapes=[pltpu.VMEM(full, f32)],
        ),
        compiler_params=pltpu.CompilerParams(
            dimension_semantics=("arbitrary",), vmem_limit_bytes=34 * 2**20
        ),
    )(picks, usable, q2, do2, kv.reshape(full))

    own = pl.pallas_call(
        functools.partial(reduce_kernel, n, SUB),
        out_shape=jax.ShapeDtypeStruct((2, tokens, width), bf16),
        in_specs=[vmem()],
        out_specs=vmem(),
        scratch_shapes=[
            pltpu.VMEM((2, half, tokens, width), bf16),
            pltpu.VMEM((2, half, tokens, width), bf16),
            pltpu.VMEM((2, half, tokens, width), bf16),
            pltpu.VMEM((2, tokens, width), bf16),
            pltpu.VMEM((2, tokens, width), bf16),
            dma((half, 2 * SUB)), dma((half, 2 * SUB)),
            dma((half,)), dma((half,)),
            dma((2 * SUB,)), dma((2 * SUB,)),
        ],
        compiler_params=pltpu.CompilerParams(
            collective_id=2, has_side_effects=True, vmem_limit_bytes=28 * 2**20
        ),
    )(tiles.reshape(2, n, tokens, width))
    gk, gv = own[0], own[1]
    return (
        dq.reshape(tokens, 1, heads_here, width),
        gk.reshape(tokens, 1, width),
        gv.reshape(tokens, 1, width),
    )


def solution(mesh):
    return jax.shard_map(
        per_device,
        mesh=mesh,
        in_specs=(
            P(("groups", "seq"), "head", "inner", None),
            P(("groups", "seq"), "head", "inner", None),
            P(("groups", "seq"), "head", None),
            P(("groups", "seq"), "head", None),
            P("head", "groups", None),
            P("head", "groups", None),
        ),
        out_specs=(
            P(("groups", "seq"), "head", "inner", None),
            P(("groups", "seq"), "head", None),
            P(("groups", "seq"), "head", None),
        ),
        check_vma=False,
    )
```

```python
import functools
import math

import jax
import jax.numpy as jnp
from jax import lax
from jax.experimental import pallas as pl
from jax.experimental.pallas import tpu as pltpu
from jax.sharding import PartitionSpec as P

BLK = 64
TOPK = 16
SUB = 4
TOGETHER = 4
MESH = pl.DeviceIdType.MESH
LOG2E = 1.4426950408889634


def greet(n):
    me = lax.axis_index("seq")
    core = lax.axis_index("inner")
    barrier = pltpu.get_barrier_semaphore()
    peers = ({"seq": lax.rem(me + 1, n)}, {"seq": lax.rem(me + n - 1, n)}, {"inner": 1 - core})
    for where in peers:
        pl.semaphore_signal(barrier, inc=1, device_id=where, device_id_type=MESH)
    pl.semaphore_wait(barrier, len(peers))


def send(src, dst, s_sem, r_sem, where):
    return pltpu.make_async_remote_copy(
        src_ref=src, dst_ref=dst, send_sem=s_sem, recv_sem=r_sem, device_id=where, device_id_type=MESH
    )


def gather_kernel(n, sub, own_ref, kv_ref, local_sem, ss, rs, ps, pr):
    me = lax.axis_index("seq")
    core = lax.axis_index("inner")
    way = 1 - 2 * core
    ahead = {"seq": lax.rem(me + way + n, n)}
    partner = {"inner": 1 - core}
    part = own_ref.shape[1] // sub
    half = n // 2
    own = pltpu.make_async_copy(own_ref, kv_ref.at[:, me], local_sem)
    own.start()
    greet(n)
    own.wait()

    def run_of(t):
        return lax.rem(me - way * t + n, n)

    def pieces(t):
        first = [(core, u, u) for u in range(sub)]
        if t == half - 1:
            return first
        return first + [(1 - core, u, sub + u) for u in range(sub)]

    def hop(t, a, u, j):
        ref = kv_ref.at[a, run_of(t), pl.ds(u * part, part)]
        return send(ref, ref, ss.at[t, j], rs.at[t, j], ahead)

    def share(t):
        if t == half:
            ref = kv_ref.at[core, run_of(t)]
        else:
            ref = kv_ref.at[:, run_of(t)]
        return send(ref, ref, ps.at[t], pr.at[t], partner)

    def landed(t):
        run = lax.rem(me + way * t + n, n)
        if t == half:
            ref = kv_ref.at[1 - core, run]
        else:
            ref = kv_ref.at[:, run]
        return send(ref, ref, ps.at[t], pr.at[t], partner)

    for p in pieces(0):
        hop(0, *p).start()
    for t in range(half):
        later = [j for _, _, j in pieces(t + 1)] if t + 1 < half else []
        for a, u, j in pieces(t):
            ref = kv_ref.at[a, run_of(t + 1), pl.ds(u * part, part)]
            send(ref, ref, ss.at[t, j], rs.at[t, j], ahead).wait_recv()
            if j in later:
                hop(t + 1, a, u, j).start()
        share(t + 1).start()
    for t in range(1, half + 1):
        landed(t).wait_recv()
        share(t).wait_send()
    for t in range(half):
        for p in pieces(t):
            hop(t, *p).wait_send()


def attend_block(scaling, at, picks, usable, q, do, kv_ref):
    rows = q.shape[0]
    per_pos = rows // BLK
    names = [jnp.where(usable[t, at] > 0, picks[t, at], at) for t in range(TOPK)]
    ks = jnp.concatenate([kv_ref[0, b] for b in names], axis=0)
    vs = jnp.concatenate([kv_ref[1, b] for b in names], axis=0)
    nt = (((1,), (1,)), ((), ()))
    st = lax.dot_general(ks, q, nt, preferred_element_type=jnp.float32)
    dp = lax.dot_general(vs, do, nt, preferred_element_type=jnp.float32)
    key_at = lax.broadcasted_iota(jnp.int32, (BLK, rows), 0)
    query_at = lax.broadcasted_iota(jnp.int32, (BLK, rows), 1) // per_pos
    low = jnp.float32(-1e30)
    parts = [jnp.where(key_at <= query_at, st[:BLK], low)]
    for t in range(1, TOPK):
        bias = jnp.where(usable[t, at] > 0, jnp.float32(0.0), low)
        parts.append(st[t * BLK : (t + 1) * BLK] + bias)
    st = jnp.concatenate(parts, axis=0)
    top = jnp.max(st, axis=0, keepdims=True)
    w = jnp.exp2((st - top) * jnp.float32(scaling * LOG2E))
    inv = 1.0 / jnp.sum(w, axis=0, keepdims=True)
    p = w * inv
    delta = jnp.sum(p * dp, axis=0, keepdims=True)
    dsc = (p * (dp - delta)).astype(jnp.bfloat16)
    pb = p.astype(jnp.bfloat16)
    dqt = lax.dot_general(ks, dsc, (((0,), (0,)), ((), ())), preferred_element_type=jnp.float32)
    dq = (dqt.T * scaling).astype(jnp.bfloat16)
    dk = jnp.dot(dsc, q, preferred_element_type=jnp.float32) * scaling
    dv = jnp.dot(pb, do, preferred_element_type=jnp.float32)
    return names, dq, dk, dv


def attend_kernel(scaling, rows, picks, usable, q_ref, do_ref, kv_ref, dq_ref, tiles_ref, acc):
    i = pl.program_id(0)
    steps = pl.num_programs(0)
    here = q_ref.shape[0] // rows
    at = (lax.axis_index("seq") * steps + i) * here

    @pl.when(i == 0)
    def _():
        acc[...] = jnp.zeros_like(acc)

    done = []
    for b in range(here):
        s = slice(b * rows, (b + 1) * rows)
        done.append(attend_block(scaling, at + b, picks, usable, q_ref[s], do_ref[s], kv_ref))
    for b in range(here):
        names, dq, dk, dv = done[b]
        dq_ref[b * rows : (b + 1) * rows] = dq
        for t in range(TOPK):
            acc[0, names[t]] += dk[t * BLK : (t + 1) * BLK]
            acc[1, names[t]] += dv[t * BLK : (t + 1) * BLK]

    @pl.when(i == steps - 1)
    def _():
        tiles_ref[...] = acc[...].astype(jnp.bfloat16)


def reduce_kernel(n, sub, tiles, out, peer, put, got, mine, theirs, ss, rs, ps, pr, fs, fr):
    me = lax.axis_index("seq")
    core = lax.axis_index("inner")
    way = 1 - 2 * core
    ahead = {"seq": lax.rem(me - way + n, n)}
    partner = {"inner": 1 - core}
    part = tiles.shape[2] // sub
    half = n // 2
    f32, bf16 = jnp.float32, jnp.bfloat16
    greet(n)

    def owner(t, way):
        return lax.rem(me - way * (half - t) + 2 * n, n)

    def hand(t):
        run = owner(t, -way)
        if t == 0:
            src, dst = tiles.at[1 - core, run], peer.at[1 - core, t]
        else:
            src, dst = tiles.at[:, run], peer.at[:, t]
        return send(src, dst, ps.at[t], pr.at[t], partner)

    def landed(t):
        if t == 0:
            ref = peer.at[core, t]
        else:
            ref = peer.at[:, t]
        return send(ref, ref, ps.at[t], pr.at[t], partner)

    def pieces(t):
        last = [(core, u, u) for u in range(sub)]
        if t == 0:
            return last
        return [(1 - core, u, sub + u) for u in range(sub)] + last

    def hop(t, a, u, j):
        s = pl.ds(u * part, part)
        return send(put.at[a, t, s], got.at[a, t, s], ss.at[t, j], rs.at[t, j], ahead)

    for t in range(half):
        hand(t).start()
    for t in range(half):
        landed(t).wait_recv()
        run = owner(t, way)
        for a, u, j in pieces(t):
            s = pl.ds(u * part, part)
            val = tiles[a, run, s, :].astype(f32) + peer[a, t, s, :].astype(f32)
            if t > 1 or (t == 1 and j < sub):
                hop(t - 1, a, u, j).wait_recv()
                val = val + got[a, t - 1, s, :].astype(f32)
            put[a, t, s, :] = val.astype(bf16)
            hop(t, a, u, j).start()
    swaps = []
    for a, u, j in pieces(half - 1):
        s = pl.ds(u * part, part)
        hop(half - 1, a, u, j).wait_recv()
        mine[a, s, :] = (tiles[a, me, s, :].astype(f32) + got[a, half - 1, s, :].astype(f32)).astype(bf16)
        c = send(mine.at[a, s], theirs.at[a, s], fs.at[a * sub + u], fr.at[a * sub + u], partner)
        c.start()
        swaps.append((c, a, s))
    for c, a, s in swaps[sub:] + swaps[:sub]:
        c.wait_recv()
        out[a, s, :] = (mine[a, s, :].astype(f32) + theirs[a, s, :].astype(f32)).astype(bf16)
    for c, a, s in swaps:
        c.wait_send()
    for t in range(half):
        hand(t).wait_send()
        for p in pieces(t):
            hop(t, *p).wait_send()


def vmem():
    return pl.BlockSpec(memory_space=pltpu.VMEM)


def anywhere():
    return pl.BlockSpec(memory_space=pl.ANY)


def per_device(queries, grad_out, keys, values, indices, valid):
    tokens, _, heads_here, width = queries.shape
    n = lax.axis_size("seq")
    blocks = tokens // BLK
    total_blocks = n * blocks
    scaling = 1.0 / math.sqrt(width)
    rows = BLK * heads_here
    half = n // 2
    dma = pltpu.SemaphoreType.DMA
    bf16, f32 = jnp.bfloat16, jnp.float32
    picks, usable = indices[0].T, valid[0].T

    kv = pl.pallas_call(
        functools.partial(gather_kernel, n, SUB),
        out_shape=jax.ShapeDtypeStruct((2, n, tokens, width), bf16),
        in_specs=[anywhere()],
        out_specs=vmem(),
        scratch_shapes=[
            dma,
            dma((half, 2 * SUB)), dma((half, 2 * SUB)),
            dma((half + 1,)), dma((half + 1,)),
        ],
        compiler_params=pltpu.CompilerParams(collective_id=1, has_side_effects=True, vmem_limit_bytes=12 * 2**20),
    )(jnp.stack([keys[:, 0], values[:, 0]]))

    q2 = queries.reshape(tokens * heads_here, width)
    do2 = grad_out.reshape(tokens * heads_here, width)
    full = (2, total_blocks, BLK, width)
    whole = lambda i, *_: (0, 0, 0, 0)
    by_block = pl.BlockSpec((TOGETHER * rows, width), lambda i, *_: (i, 0))
    dq, tiles = pl.pallas_call(
        functools.partial(attend_kernel, scaling, rows),
        out_shape=(
            jax.ShapeDtypeStruct((tokens * heads_here, width), bf16),
            jax.ShapeDtypeStruct(full, bf16),
        ),
        grid_spec=pltpu.PrefetchScalarGridSpec(
            num_scalar_prefetch=2,
            grid=(blocks // TOGETHER,),
            in_specs=[by_block, by_block, pl.BlockSpec(full, whole)],
            out_specs=[by_block, pl.BlockSpec(full, whole)],
            scratch_shapes=[pltpu.VMEM(full, f32)],
        ),
        compiler_params=pltpu.CompilerParams(
            dimension_semantics=("arbitrary",), vmem_limit_bytes=34 * 2**20
        ),
    )(picks, usable, q2, do2, kv.reshape(full))

    own = pl.pallas_call(
        functools.partial(reduce_kernel, n, SUB),
        out_shape=jax.ShapeDtypeStruct((2, tokens, width), bf16),
        in_specs=[vmem()],
        out_specs=vmem(),
        scratch_shapes=[
            pltpu.VMEM((2, half, tokens, width), bf16),
            pltpu.VMEM((2, half, tokens, width), bf16),
            pltpu.VMEM((2, half, tokens, width), bf16),
            pltpu.VMEM((2, tokens, width), bf16),
            pltpu.VMEM((2, tokens, width), bf16),
            dma((half, 2 * SUB)), dma((half, 2 * SUB)),
            dma((half,)), dma((half,)),
            dma((2 * SUB,)), dma((2 * SUB,)),
        ],
        compiler_params=pltpu.CompilerParams(
            collective_id=2, has_side_effects=True, vmem_limit_bytes=28 * 2**20
        ),
    )(tiles.reshape(2, n, tokens, width))
    gk, gv = own[0], own[1]
    return (
        dq.reshape(tokens, 1, heads_here, width),
        gk.reshape(tokens, 1, width),
        gv.reshape(tokens, 1, width),
    )


def solution(mesh):
    return jax.shard_map(
        per_device,
        mesh=mesh,
        in_specs=(
            P(("groups", "seq"), "head", "inner", None),
            P(("groups", "seq"), "head", "inner", None),
            P(("groups", "seq"), "head", None),
            P(("groups", "seq"), "head", None),
            P("head", "groups", None),
            P("head", "groups", None),
        ),
        out_specs=(
            P(("groups", "seq"), "head", "inner", None),
            P(("groups", "seq"), "head", None),
            P(("groups", "seq"), "head", None),
        ),
        check_vma=False,
    )
```

```python
import functools
import math

import jax
import jax.numpy as jnp
from jax import lax
from jax.experimental import pallas as pl
from jax.experimental.pallas import tpu as pltpu
from jax.sharding import PartitionSpec as P

BLK = 64
TOPK = 16
SUB = 8
COARSE = 2
TOGETHER = 4
MESH = pl.DeviceIdType.MESH
LOG2E = 1.4426950408889634


def greet(n):
    me = lax.axis_index("seq")
    core = lax.axis_index("inner")
    barrier = pltpu.get_barrier_semaphore()
    peers = ({"seq": lax.rem(me + 1, n)}, {"seq": lax.rem(me + n - 1, n)}, {"inner": 1 - core})
    for where in peers:
        pl.semaphore_signal(barrier, inc=1, device_id=where, device_id_type=MESH)
    pl.semaphore_wait(barrier, len(peers))


def send(src, dst, s_sem, r_sem, where):
    return pltpu.make_async_remote_copy(
        src_ref=src, dst_ref=dst, send_sem=s_sem, recv_sem=r_sem, device_id=where, device_id_type=MESH
    )


def cut(a, rows, count, j):
    size = rows // count
    return [(a, pl.ds(u * size, size), j + u) for u in range(count)]


def gather_kernel(n, sub, own_ref, kv_ref, local_sem, ss, rs, ps, pr):
    me = lax.axis_index("seq")
    core = lax.axis_index("inner")
    way = 1 - 2 * core
    ahead = {"seq": lax.rem(me + way + n, n)}
    partner = {"inner": 1 - core}
    rows = own_ref.shape[1]
    half = n // 2
    own = pltpu.make_async_copy(own_ref, kv_ref.at[:, me], local_sem)
    own.start()
    greet(n)
    own.wait()

    def run_of(t):
        return lax.rem(me - way * t + n, n)

    def pieces(t):
        first = cut(core, rows, sub, 0)
        if t == half - 1:
            return first
        return first + cut(1 - core, rows, COARSE, sub)

    def hop(t, a, s, j):
        ref = kv_ref.at[a, run_of(t), s]
        return send(ref, ref, ss.at[t, j], rs.at[t, j], ahead)

    def share(t):
        if t == half:
            ref = kv_ref.at[core, run_of(t)]
        else:
            ref = kv_ref.at[:, run_of(t)]
        return send(ref, ref, ps.at[t], pr.at[t], partner)

    def landed(t):
        run = lax.rem(me + way * t + n, n)
        if t == half:
            ref = kv_ref.at[1 - core, run]
        else:
            ref = kv_ref.at[:, run]
        return send(ref, ref, ps.at[t], pr.at[t], partner)

    for p in pieces(0):
        hop(0, *p).start()
    for t in range(half):
        later = [j for _, _, j in pieces(t + 1)] if t + 1 < half else []
        for a, s, j in pieces(t):
            ref = kv_ref.at[a, run_of(t + 1), s]
            send(ref, ref, ss.at[t, j], rs.at[t, j], ahead).wait_recv()
            if j in later:
                hop(t + 1, a, s, j).start()
        share(t + 1).start()
    for t in range(1, half + 1):
        landed(t).wait_recv()
        share(t).wait_send()
    for t in range(half):
        for p in pieces(t):
            hop(t, *p).wait_send()


def attend_block(scaling, at, picks, usable, q, do, kv_ref):
    rows = q.shape[0]
    per_pos = rows // BLK
    names = [jnp.where(usable[t, at] > 0, picks[t, at], at) for t in range(TOPK)]
    ks = jnp.concatenate([kv_ref[0, b] for b in names], axis=0)
    vs = jnp.concatenate([kv_ref[1, b] for b in names], axis=0)
    nt = (((1,), (1,)), ((), ()))
    st = lax.dot_general(ks, q, nt, preferred_element_type=jnp.float32)
    dp = lax.dot_general(vs, do, nt, preferred_element_type=jnp.float32)
    key_at = lax.broadcasted_iota(jnp.int32, (BLK, rows), 0)
    query_at = lax.broadcasted_iota(jnp.int32, (BLK, rows), 1) // per_pos
    low = jnp.float32(-1e30)
    parts = [jnp.where(key_at <= query_at, st[:BLK], low)]
    for t in range(1, TOPK):
        bias = jnp.where(usable[t, at] > 0, jnp.float32(0.0), low)
        parts.append(st[t * BLK : (t + 1) * BLK] + bias)
    st = jnp.concatenate(parts, axis=0)
    top = jnp.max(st, axis=0, keepdims=True)
    w = jnp.exp2((st - top) * jnp.float32(scaling * LOG2E))
    inv = 1.0 / jnp.sum(w, axis=0, keepdims=True)
    p = w * inv
    delta = jnp.sum(p * dp, axis=0, keepdims=True)
    dsc = (p * (dp - delta)).astype(jnp.bfloat16)
    pb = p.astype(jnp.bfloat16)
    dqt = lax.dot_general(ks, dsc, (((0,), (0,)), ((), ())), preferred_element_type=jnp.float32)
    dq = (dqt.T * scaling).astype(jnp.bfloat16)
    dk = jnp.dot(dsc, q, preferred_element_type=jnp.float32) * scaling
    dv = jnp.dot(pb, do, preferred_element_type=jnp.float32)
    return names, dq, dk, dv


def attend_kernel(scaling, rows, picks, usable, q_ref, do_ref, kv_ref, dq_ref, tiles_ref, acc):
    i = pl.program_id(0)
    steps = pl.num_programs(0)
    here = q_ref.shape[0] // rows
    at = (lax.axis_index("seq") * steps + i) * here

    @pl.when(i == 0)
    def _():
        acc[...] = jnp.zeros_like(acc)

    done = []
    for b in range(here):
        s = slice(b * rows, (b + 1) * rows)
        done.append(attend_block(scaling, at + b, picks, usable, q_ref[s], do_ref[s], kv_ref))
    for b in range(here):
        names, dq, dk, dv = done[b]
        dq_ref[b * rows : (b + 1) * rows] = dq
        for t in range(TOPK):
            acc[0, names[t]] += dk[t * BLK : (t + 1) * BLK]
            acc[1, names[t]] += dv[t * BLK : (t + 1) * BLK]

    @pl.when(i == steps - 1)
    def _():
        tiles_ref[...] = acc[...].astype(jnp.bfloat16)


def reduce_kernel(n, sub, tiles, out, peer, put, got, mine, theirs, ss, rs, ps, pr, fs, fr):
    me = lax.axis_index("seq")
    core = lax.axis_index("inner")
    way = 1 - 2 * core
    ahead = {"seq": lax.rem(me - way + n, n)}
    partner = {"inner": 1 - core}
    rows = tiles.shape[2]
    half = n // 2
    f32, bf16 = jnp.float32, jnp.bfloat16
    greet(n)

    def owner(t, way):
        return lax.rem(me - way * (half - t) + 2 * n, n)

    def hand(t):
        run = owner(t, -way)
        if t == 0:
            src, dst = tiles.at[1 - core, run], peer.at[1 - core, t]
        else:
            src, dst = tiles.at[:, run], peer.at[:, t]
        return send(src, dst, ps.at[t], pr.at[t], partner)

    def landed(t):
        if t == 0:
            ref = peer.at[core, t]
        else:
            ref = peer.at[:, t]
        return send(ref, ref, ps.at[t], pr.at[t], partner)

    def pieces(t):
        last = cut(core, rows, sub, 0)
        if t == 0:
            return last
        return cut(1 - core, rows, COARSE, sub) + last

    def hop(t, a, s, j):
        return send(put.at[a, t, s], got.at[a, t, s], ss.at[t, j], rs.at[t, j], ahead)

    for t in range(half):
        hand(t).start()
    for t in range(half):
        landed(t).wait_recv()
        run = owner(t, way)
        for a, s, j in pieces(t):
            val = tiles[a, run, s, :].astype(f32) + peer[a, t, s, :].astype(f32)
            if t > 1 or (t == 1 and j < sub):
                hop(t - 1, a, s, j).wait_recv()
                val = val + got[a, t - 1, s, :].astype(f32)
            put[a, t, s, :] = val.astype(bf16)
            hop(t, a, s, j).start()
    def swap(a):
        return send(mine.at[a], theirs.at[a], fs.at[a], fr.at[a], partner)

    for a, s, j in pieces(half - 1):
        hop(half - 1, a, s, j).wait_recv()
        mine[a, s, :] = (tiles[a, me, s, :].astype(f32) + got[a, half - 1, s, :].astype(f32)).astype(bf16)
        if j == sub + COARSE - 1:
            swap(1 - core).start()
    swap(core).start()
    for a in (core, 1 - core):
        swap(a).wait_recv()
        out[a] = (mine[a].astype(f32) + theirs[a].astype(f32)).astype(bf16)
    for a in range(2):
        swap(a).wait_send()
    for t in range(half):
        hand(t).wait_send()
        for p in pieces(t):
            hop(t, *p).wait_send()


def vmem():
    return pl.BlockSpec(memory_space=pltpu.VMEM)


def anywhere():
    return pl.BlockSpec(memory_space=pl.ANY)


def per_device(queries, grad_out, keys, values, indices, valid):
    tokens, _, heads_here, width = queries.shape
    n = lax.axis_size("seq")
    blocks = tokens // BLK
    total_blocks = n * blocks
    scaling = 1.0 / math.sqrt(width)
    rows = BLK * heads_here
    half = n // 2
    dma = pltpu.SemaphoreType.DMA
    bf16, f32 = jnp.bfloat16, jnp.float32
    picks, usable = indices[0].T, valid[0].T

    kv = pl.pallas_call(
        functools.partial(gather_kernel, n, SUB),
        out_shape=jax.ShapeDtypeStruct((2, n, tokens, width), bf16),
        in_specs=[anywhere()],
        out_specs=vmem(),
        scratch_shapes=[
            dma,
            dma((half, 2 * SUB)), dma((half, 2 * SUB)),
            dma((half + 1,)), dma((half + 1,)),
        ],
        compiler_params=pltpu.CompilerParams(collective_id=1, has_side_effects=True, vmem_limit_bytes=12 * 2**20),
    )(jnp.stack([keys[:, 0], values[:, 0]]))

    q2 = queries.reshape(tokens * heads_here, width)
    do2 = grad_out.reshape(tokens * heads_here, width)
    full = (2, total_blocks, BLK, width)
    whole = lambda i, *_: (0, 0, 0, 0)
    by_block = pl.BlockSpec((TOGETHER * rows, width), lambda i, *_: (i, 0))
    dq, tiles = pl.pallas_call(
        functools.partial(attend_kernel, scaling, rows),
        out_shape=(
            jax.ShapeDtypeStruct((tokens * heads_here, width), bf16),
            jax.ShapeDtypeStruct(full, bf16),
        ),
        grid_spec=pltpu.PrefetchScalarGridSpec(
            num_scalar_prefetch=2,
            grid=(blocks // TOGETHER,),
            in_specs=[by_block, by_block, pl.BlockSpec(full, whole)],
            out_specs=[by_block, pl.BlockSpec(full, whole)],
            scratch_shapes=[pltpu.VMEM(full, f32)],
        ),
        compiler_params=pltpu.CompilerParams(
            dimension_semantics=("arbitrary",), vmem_limit_bytes=34 * 2**20
        ),
    )(picks, usable, q2, do2, kv.reshape(full))

    own = pl.pallas_call(
        functools.partial(reduce_kernel, n, SUB),
        out_shape=jax.ShapeDtypeStruct((2, tokens, width), bf16),
        in_specs=[vmem()],
        out_specs=vmem(),
        scratch_shapes=[
            pltpu.VMEM((2, half, tokens, width), bf16),
            pltpu.VMEM((2, half, tokens, width), bf16),
            pltpu.VMEM((2, half, tokens, width), bf16),
            pltpu.VMEM((2, tokens, width), bf16),
            pltpu.VMEM((2, tokens, width), bf16),
            dma((half, 2 * SUB)), dma((half, 2 * SUB)),
            dma((half,)), dma((half,)),
            dma((2,)), dma((2,)),
        ],
        compiler_params=pltpu.CompilerParams(
            collective_id=2, has_side_effects=True, vmem_limit_bytes=28 * 2**20
        ),
    )(tiles.reshape(2, n, tokens, width))
    gk, gv = own[0], own[1]
    return (
        dq.reshape(tokens, 1, heads_here, width),
        gk.reshape(tokens, 1, width),
        gv.reshape(tokens, 1, width),
    )


def solution(mesh):
    return jax.shard_map(
        per_device,
        mesh=mesh,
        in_specs=(
            P(("groups", "seq"), "head", "inner", None),
            P(("groups", "seq"), "head", "inner", None),
            P(("groups", "seq"), "head", None),
            P(("groups", "seq"), "head", None),
            P("head", "groups", None),
            P("head", "groups", None),
        ),
        out_specs=(
            P(("groups", "seq"), "head", "inner", None),
            P(("groups", "seq"), "head", None),
            P(("groups", "seq"), "head", None),
        ),
        check_vma=False,
    )
```
